256 devices in a mesh: ex: 32 (over x, y, core), cls: 8 (over z).
Axes of the slice: x: 4, y: 4, z: 8, core: 2. Of those that a mesh axis runs over, the one named last changes fastest.
Arguments:
- features: bfloat16 [32768, 1664], P('ex'), may hold values from -16 to 16
- labels: int32 [32768], P('ex'), may hold values from 0 to 11263
- weight: bfloat16 [1664, 11264], P(None, 'cls'), may hold values from -1 to 1
- noise: bfloat16 [1664, 11264], P('ex', 'cls'), may hold values from -5 to 5
Outputs:
- new_weight: bfloat16 [1664, 11264], P(None, 'cls')
The draws below stay inside these ranges and needn't reach their ends.
All inputs are finite; a program needn't handle non-finite values.
Results may differ from the reference program's by a relative error of at most 0.0013.
Values may be sent and summed in bfloat16 or wider, within the bound.
A program may use at most 128 MiB of HBM per device.

```python
import jax
import jax.numpy as jnp
from jax import lax

D = 1664
B_DEV = 1024
CLASSES = 11264
BATCH = 32768
N_EX = 32


def shared_weight(key):
    base = jax.random.normal(jax.random.fold_in(key, 11), (D, CLASSES), jnp.float32)
    return jnp.clip(base * (9.0 / D) ** 0.5, -1.0, 1.0)


def draw_weight(key, part):
    return shared_weight(key).astype(jnp.bfloat16)


def draw_features(key, part):
    table = shared_weight(key).astype(jnp.bfloat16).astype(jnp.float32)
    drawn = jnp.clip(jax.random.normal(jax.random.fold_in(key, 12), (BATCH, D), jnp.float32), -6.0, 6.0)
    first = jax.random.randint(jax.random.fold_in(key, 14), (BATCH,), 0, CLASSES)
    second = (first + 1 + jax.random.randint(jax.random.fold_in(key, 15), (BATCH,), 0, CLASSES - 1)) % CLASSES
    row_ids = jnp.arange(BATCH, dtype=jnp.int32)
    strength = 110.0 + 105.0 * (row_ids // 64 % 3).astype(jnp.float32)
    picked = (row_ids % 64 == 5) | (row_ids % 64 == 37)
    col_a = jnp.take(table, first, axis=1).T
    col_b = jnp.take(table, second, axis=1).T
    aligned = (strength[:, None] * col_a + (strength[:, None] - 2.0) * col_b) / 9.0 + 0.05 * drawn
    result = jnp.where(picked[:, None], aligned, drawn)
    return jnp.clip(result, -16.0, 16.0).astype(jnp.bfloat16)


def plant(drawn, stream_key, least, largest):
    shape = drawn.shape
    spot = [jax.random.randint(jax.random.fold_in(stream_key, axis), (), 0, shape[axis]) for axis in range(len(shape))]
    drawn = drawn.at[tuple(spot)].set(least)
    longest = shape.index(max(shape))
    spot[longest] = (spot[longest] + 1) % shape[longest]
    return drawn.at[tuple(spot)].set(largest)


def level_of(rng, shape, cuts, smallest, high):
    def one(position, parts):
        steps = jax.random.uniform(jax.random.fold_in(jax.random.fold_in(rng, 6), position), (parts,), jnp.float32, smallest / len(cuts), high / len(cuts))
        return jnp.repeat(jnp.exp(steps), shape[position] // parts).reshape((-1,) + (1,) * (len(shape) - position - 1))

    gain = one(*cuts[0])
    for cut in cuts[1:]:
        gain = gain * one(*cut)
    return gain


def gaussian(stream_key, shape, deviation, bound, cuts=(), kind=jnp.bfloat16):
    values = deviation * jax.random.normal(stream_key, shape, jnp.float32)
    if cuts:
        values = values * level_of(stream_key, shape, cuts, -0.22, 0.18)
    return jnp.clip(values, -bound, bound).astype(kind)


def setup_inputs(seed: int = 0) -> dict:
    arg_keys = jax.random.split(jax.random.key(seed), 5)
    return {
        "features": draw_features(jax.random.fold_in(arg_keys[4], 71), 0),
        "labels": plant(jax.random.randint(arg_keys[1], (BATCH,), 0, CLASSES), jax.random.fold_in(arg_keys[1], 1), 0, CLASSES - 1).astype(jnp.int32),
        "weight": draw_weight(jax.random.fold_in(arg_keys[4], 71), 0),
        "noise": gaussian(arg_keys[3], (D, CLASSES), 1.0, 5.0, ((0, 32), (1, 8))),
    }


def reference(features, labels, weight, noise):
    clip_norm = 48.0
    blocks_x = features.reshape(N_EX, B_DEV, D)
    blocks_l = labels.reshape(N_EX, B_DEV)
    classes_row = jnp.arange(CLASSES, dtype=jnp.int32)

    def accumulate(total, item):
        rows, labs = item
        logits = jnp.dot(rows, weight, preferred_element_type=jnp.float32)
        probs = jax.nn.softmax(logits, axis=1)
        onehot = (classes_row[None, :] == labs[:, None]).astype(jnp.float32)
        resid = probs - onehot
        resid_norm = jnp.sqrt(lax.optimization_barrier(jnp.sum(resid * resid, axis=1)))
        feat = rows.astype(jnp.float32)
        feat_norm = jnp.sqrt(lax.optimization_barrier(jnp.sum(feat * feat, axis=1)))
        factor = clip_norm / jnp.maximum(feat_norm * resid_norm, clip_norm)
        coef = (factor[:, None] * resid).astype(jnp.bfloat16)
        part = lax.dot_general(rows, coef, (((0,), (0,)), ((), ())), preferred_element_type=jnp.float32)
        return (total + part, None)
    grad, _ = lax.scan(accumulate, jnp.zeros((D, CLASSES), jnp.float32), (blocks_x, blocks_l))
    scale = 0.1 * CLASSES / BATCH
    updated = weight.astype(jnp.float32) - scale * (grad + 0.96 * clip_norm * noise.astype(jnp.float32))
    return updated.astype(jnp.bfloat16)
```

```python
import functools

import jax
import jax.numpy as jnp
from jax import lax
from jax.experimental import pallas as pl
from jax.experimental.pallas import tpu as pltpu
from jax.sharding import PartitionSpec as P

MESH = pl.DeviceIdType.MESH
F32, BF16 = jnp.float32, jnp.bfloat16
CLIP = 48.0
WIDE = 256
LANES = 128
CUT = 48
ROWS = ((0, 48), (48, 56))


def kernel(scale, f_hbm, lab_ref, w_hbm, noise_hbm, out_ref,
           f_v, w_v, ft_v, e_v, coef_v, lab_v, xt_v, st_v, fn_v, psend_v, precv_v,
           g_v, ra_v, hf_v, hs_v, rb_v, base_v, wown_v, nz_v,
           ld_sem, st_s, st_r, nz_s, nz_r, p_s, p_r, a_s, a_r, b_s, b_r,
           g1_s, g1_r, g2_s, g2_r, g3_s, g3_r, d_s, d_r):
    rows, depth = f_hbm.shape
    width = w_hbm.shape[1]
    n_cls = lax.axis_size("cls")
    ex = lax.axis_index("ex")
    z = lax.axis_index("cls")
    c = ex % 2
    x = ex // 8
    y = (ex // 2) % 4
    a = x * (1 - c) + y * c
    b = y * (1 - c) + x * c

    def spot(i, j):
        return i * (4 - 3 * c) + j * (1 + 3 * c)

    def dev(i, j):
        return spot(i, j) * 2 + c

    mine = spot(a, b)
    a_up, a_dn, a_op = (a + 1) % 4, (a + 3) % 4, (a + 2) % 4
    b_up, b_dn, b_op = (b + 1) % 4, (b + 3) % 4, (b + 2) % 4
    to_aup, to_adn = dev(a_up, b), dev(a_dn, b)
    to_bup, to_bdn = dev(a, b_up), dev(a, b_dn)
    partner = ex + 1 - 2 * c

    barrier = pltpu.get_barrier_semaphore()
    for t in (to_aup, to_adn, to_bup, to_bdn, partner):
        pl.semaphore_signal(barrier, inc=1, device_id={"ex": t}, device_id_type=MESH)
    for k in range(1, n_cls):
        pl.semaphore_signal(barrier, inc=1, device_id={"cls": (z + k) % n_cls}, device_id_type=MESH)

    def send(src, dst, s, r, t):
        return pltpu.make_async_remote_copy(
            src_ref=src, dst_ref=dst, send_sem=s, recv_sem=r, device_id={"ex": t}, device_id_type=MESH)

    loads = [
        pltpu.make_async_copy(f_hbm, f_v, ld_sem.at[0]),
        pltpu.make_async_copy(w_hbm, w_v, ld_sem.at[1]),
        pltpu.make_async_copy(w_hbm.at[pl.ds(pl.multiple_of(mine * 104, 8), 104), :], wown_v, ld_sem.at[2]),
        pltpu.make_async_copy(noise_hbm, nz_v.at[c], ld_sem.at[3]),
    ]
    for cp in loads:
        cp.start()

    for i in range(rows // LANES):
        row = jnp.broadcast_to(lab_ref[i:i + 1, :].astype(F32), (LANES, LANES))
        lab_v[i * LANES:(i + 1) * LANES, :] = row.T.astype(jnp.int32) - z * width
    lane = lax.broadcasted_iota(jnp.int32, (64, LANES), 1)

    for cp in loads:
        cp.wait()
    pl.semaphore_wait(barrier, 5 + n_cls - 1)
    nz = send(noise_hbm, nz_v.at[c], nz_s, nz_r, partner)
    nz.start()

    tiles = width // LANES

    def st_copy(blk, k):
        return pltpu.make_async_remote_copy(
            src_ref=st_v.at[z, blk], dst_ref=st_v.at[z, blk], send_sem=st_s.at[blk, k - 1],
            recv_sem=st_r.at[blk, k - 1], device_id={"cls": (z + k) % n_cls}, device_id_type=MESH)

    def forward(blk, _):
        r256 = pl.ds(pl.multiple_of(blk * 256, 256), 256)
        for n in range(0, width, WIDE):
            w = min(WIDE, width - n)
            e_v[r256, n:n + w] = jnp.dot(f_v[r256, :], w_v[:, n:n + w], preferred_element_type=F32)
        for h in range(2):
            r128 = pl.ds(pl.multiple_of(blk * 256 + h * 128, 128), 128)
            ft_v[:, r128] = f_v[r128, :].T
            for s in range(2):
                r = pl.ds(pl.multiple_of(blk * 256 + h * 128 + s * 64, 64), 64)
                top = e_v[r, 0:LANES]
                for n in range(1, tiles):
                    top = jnp.maximum(top, e_v[r, n * LANES:(n + 1) * LANES])
                top = jnp.max(top, axis=1, keepdims=True)
                lab = lab_v[r, :]
                one = jnp.zeros((64, LANES), F32)
                two, hit, sq = one, one, one
                for n in range(tiles):
                    cols = slice(n * LANES, (n + 1) * LANES)
                    v = jnp.exp(e_v[r, cols] - top)
                    e_v[r, cols] = v
                    one += v
                    two += v * v
                    hit += jnp.where(lane + n * LANES == lab, v, 0.0)
                for k in range(depth // LANES):
                    v = f_v[r, k * LANES:(k + 1) * LANES].astype(F32)
                    sq += v * v
                one = jnp.sum(one, axis=1, keepdims=True)
                two = jnp.sum(two, axis=1, keepdims=True)
                hit = jnp.sum(hit, axis=1, keepdims=True)
                sq = jnp.sum(sq, axis=1, keepdims=True)
                pick = jnp.where(lane == 4 * h, top, 0.0)
                pick = jnp.where(lane == 4 * h + 1, one, pick)
                pick = jnp.where(lane == 4 * h + 2, two, pick)
                pick = jnp.where(lane == 4 * h + 3, hit, pick)
                pick = jnp.where(lane == 8 + h, sq, pick)
                if h == 0:
                    xt_v[s * 64:(s + 1) * 64, :] = pick
                else:
                    xt_v[s * 64:(s + 1) * 64, :] += pick
        t = xt_v[...].T
        st_v[z, blk] = t[0:8]
        fn_v[blk] = t[8:16]
        for k in range(1, n_cls):
            st_copy(blk, k).start()
        return 0

    lax.fori_loop(0, rows // 256, forward, 0)

    nz.wait_recv()
    for n in range(0, width, WIDE):
        w = min(WIDE, width - n)
        base_v[n // WIDE, :, 0:w] = wown_v[:, n:n + w].astype(F32)
        for i in range(2):
            base_v[n // WIDE, i * 52:(i + 1) * 52, 0:w] -= (scale * 0.96 * CLIP) * nz_v[i, :, n:n + w].astype(F32)

    def weigh(blk, _):
        for k in range(1, n_cls):
            st_copy(blk, k).wait_recv()
        for h in range(2):
            tops = [st_v[p, blk, 4 * h:4 * h + 1, :] for p in range(n_cls)]
            top = functools.reduce(jnp.maximum, tops)
            total = jnp.zeros((1, LANES), F32)
            squares, hit = total, total
            for p in range(n_cls):
                g = jnp.exp(tops[p] - top)
                total += st_v[p, blk, 4 * h + 1:4 * h + 2, :] * g
                squares += st_v[p, blk, 4 * h + 2:4 * h + 3, :] * (g * g)
                hit += st_v[p, blk, 4 * h + 3:4 * h + 4, :] * g
            prob = hit / total
            miss = 1.0 - prob
            resid = jnp.maximum(squares / (total * total) - prob * prob, 0.0) + miss * miss
            norm = jnp.sqrt(fn_v[blk, h:h + 1, :]) * jnp.sqrt(resid)
            factor = CLIP / jnp.maximum(norm, CLIP)
            up = factor * jnp.exp(st_v[z, blk, 4 * h:4 * h + 1, :] - top) / total
            up = jnp.broadcast_to(up, (LANES, LANES)).T
            down = jnp.broadcast_to(factor, (LANES, LANES)).T
            for s in range(2):
                r = pl.ds(pl.multiple_of(blk * 256 + h * 128 + s * 64, 64), 64)
                lab = lab_v[r, :]
                u, d = up[s * 64:(s + 1) * 64], down[s * 64:(s + 1) * 64]
                for n in range(tiles):
                    v = e_v[r, n * LANES:(n + 1) * LANES] * u
                    v -= jnp.where(lane + n * LANES == lab, d, 0.0)
                    coef_v[n // 2, r, (n % 2) * LANES:(n % 2 + 1) * LANES] = v.astype(BF16)
        return 0

    lax.fori_loop(0, rows // 256, weigh, 0)

    def tile_of(t):
        return pl.ds(pl.multiple_of(t * 416, 32), 416)

    def p_send(j, w):
        return send(psend_v.at[j, :, pl.ds(0, w)], precv_v.at[j, :, pl.ds(0, w)], p_s.at[j], p_r.at[j], partner)

    def part(j, w, wp):
        def body(t, _):
            psend_v[j, tile_of(t), 0:wp] = jnp.dot(
                ft_v[tile_of(t), :], coef_v[(1 - c) * 3 + j, :, 0:wp], preferred_element_type=F32)
            return 0
        lax.fori_loop(0, 4, body, 0)
        p_send(j, wp).start()

    def a_msg(j, w, k):
        group, half, t = ((a_op, 0, to_aup), (a_op, 1, to_adn), (a_up, 1, to_aup),
                          (a_dn, 0, to_adn), (a_up, 0, to_aup), (a_dn, 1, to_adn))[k]
        return send(g_v.at[j, group, pl.ds(2 * half, 2), :, pl.ds(0, w)], ra_v.at[j, k, :, :, pl.ds(0, w)],
                    a_s.at[j, k], a_r.at[j, k], t)

    def own(j, w, wp):
        p_send(j, w).wait_recv()

        def body(t, _):
            acc = jnp.dot(ft_v[tile_of(t), :], coef_v[c * 3 + j, :, 0:w], preferred_element_type=F32)
            acc += precv_v[j, tile_of(t), 0:w]
            for i in range(4):
                q = spot(t, i)
                g_v[j, q // 4, q % 4, :, 0:w] = acc[i * 104:(i + 1) * 104].astype(BF16)
            return 0
        lax.fori_loop(0, 4, body, 0)
        for k in range(4):
            a_msg(j, w, k).start()

    def r1(j, w, wp):
        for k, group, half in ((0, a_up, 0), (1, a_dn, 1)):
            a_msg(j, w, k).wait_recv()
            for i in range(2):
                v = g_v[j, group, 2 * half + i, :, 0:w].astype(F32) + ra_v[j, k, i, :, 0:w].astype(F32)
                g_v[j, group, 2 * half + i, :, 0:w] = v.astype(BF16)
            a_msg(j, w, 4 + k).start()

    def b_msg(j, w, k):
        piece, half, t = ((b_op, 0, to_bup), (b_op, 1, to_bdn), (b_up, 1, to_bup),
                          (b_dn, 0, to_bdn), (b_up, 0, to_bup), (b_dn, 1, to_bdn))[k]
        r0, nr = ROWS[half]
        return send(hs_v.at[j, piece, pl.ds(r0, nr), pl.ds(0, w)], rb_v.at[j, k, pl.ds(0, nr), pl.ds(0, w)],
                    b_s.at[j, k], b_r.at[j, k], t)

    def r2(j, w, wp):
        for k in (2, 3, 4, 5):
            a_msg(j, w, k).wait_recv()
        for half, dep, ind in ((0, 4, 3), (1, 5, 2)):
            for i in range(2):
                piece = 2 * half + i
                v = g_v[j, a, piece, :, 0:w].astype(F32) + ra_v[j, dep, i, :, 0:w].astype(F32)
                v += ra_v[j, ind, i, :, 0:w].astype(F32)
                hf_v[j, piece, :, 0:w] = v
                hs_v[j, piece, :, 0:w] = v.astype(BF16)
        for k in range(4):
            b_msg(j, w, k).start()

    def r3(j, w, wp):
        for k, piece, half in ((0, b_up, 0), (1, b_dn, 1)):
            r0, nr = ROWS[half]
            b_msg(j, w, k).wait_recv()
            v = hf_v[j, piece, r0:r0 + nr, 0:w] + rb_v[j, k, 0:nr, 0:w].astype(F32)
            hs_v[j, piece, r0:r0 + nr, 0:w] = v.astype(BF16)
            b_msg(j, w, 4 + k).start()

    def cols(j, w, core):
        return pl.ds(pl.multiple_of(core * 3 * WIDE + j * WIDE, LANES), w)

    def place(j, w, p, core, half=None):
        if half is None:
            return out_ref.at[p, :, cols(j, w, core)]
        return out_ref.at[p, pl.ds(*ROWS[half]), cols(j, w, core)]

    def g1(j, w, k):
        piece, half, t = ((mine, None, to_bup), (mine, None, to_bdn),
                          (spot(a, b_dn), 0, to_bup), (spot(a, b_up), 1, to_bdn))[k]
        ref = place(j, w, piece, c, half)
        return send(ref, ref, g1_s.at[j, k], g1_r.at[j, k], t)

    near = (b, b_dn, b_up, b_op)

    def g2(j, w, r, up):
        ref = place(j, w, spot(a, near[r]), c)
        return send(ref, ref, g2_s.at[j, 2 * r + up], g2_r.at[j, 2 * r + up], to_aup if up else to_adn)

    def g3(j, w, r):
        ref = place(j, w, spot(a_dn if r < 2 else a_up, near[r]), c)
        return send(ref, ref, g3_s.at[j, r], g3_r.at[j, r], to_aup if r < 2 else to_adn)

    def d2d(j, w, i, r, core):
        ref = place(j, w, spot((a, a_dn, a_up, a_op)[i], near[r]), core)
        return send(ref, ref, d_s.at[j, 4 * i + r], d_r.at[j, 4 * i + r], partner)

    def have(j, w, r):
        g2(j, w, r, 1).start()
        g2(j, w, r, 0).start()
        d2d(j, w, 0, r, c).start()

    def u(j, w, wp):
        for k in (2, 3, 4, 5):
            b_msg(j, w, k).wait_recv()
        for half, dep, ind in ((0, 4, 3), (1, 5, 2)):
            r0, nr = ROWS[half]
            v = hf_v[j, b, r0:r0 + nr, 0:w] + rb_v[j, dep, 0:nr, 0:w].astype(F32)
            v += rb_v[j, ind, 0:nr, 0:w].astype(F32)
            v = base_v[c * 3 + j, r0:r0 + nr, 0:w] - scale * v
            out_ref[mine, r0:r0 + nr, cols(j, w, c)] = v.astype(BF16)
        g1(j, w, 0).start()
        g1(j, w, 1).start()
        have(j, w, 0)

    def a1(j, w, wp):
        g1(j, w, 0).wait_recv()
        g1(j, w, 2).start()
        g1(j, w, 1).wait_recv()
        g1(j, w, 3).start()
        have(j, w, 1)
        have(j, w, 2)

    def a2(j, w, wp):
        g1(j, w, 2).wait_recv()
        g1(j, w, 3).wait_recv()
        have(j, w, 3)

    def a3(j, w, wp):
        for r in range(4):
            g2(j, w, r, 1).wait_recv()
            if r < 2:
                g3(j, w, r).start()
            d2d(j, w, 1, r, c).start()
            g2(j, w, r, 0).wait_recv()
            if r >= 2:
                g3(j, w, r).start()
            d2d(j, w, 2, r, c).start()

    def a4(j, w, wp):
        for r in range(4):
            g3(j, w, r).wait_recv()
            d2d(j, w, 3, r, c).start()

    def last(j, w, wp):
        for i in range(4):
            for r in range(4):
                d2d(j, wp, i, r, 1 - c).wait_recv()
                d2d(j, w, i, r, c).wait_send()
        p_send(j, wp).wait_send()
        for k in range(6):
            a_msg(j, w, k).wait_send()
            b_msg(j, w, k).wait_send()
        for k in range(4):
            g1(j, w, k).wait_send()
            g3(j, w, k).wait_send()
            g2(j, w, k, 0).wait_send()
            g2(j, w, k, 1).wait_send()

    def run(fn, j):
        if j < 2:
            fn(j, WIDE, WIDE)
        else:
            @pl.when(c == 0)
            def _():
                fn(2, WIDE, LANES)

            @pl.when(c == 1)
            def _():
                fn(2, LANES, WIDE)

    order = [(part, 0), (part, 1), (own, 0), (part, 2), (own, 1), (r1, 0), (own, 2), (r1, 1), (r2, 0), (r1, 2),
             (r3, 0), (r2, 1), (u, 0), (r3, 1), (r2, 2), (a1, 0), (u, 1), (r3, 2), (a2, 0), (a1, 1), (u, 2),
             (a2, 1), (a1, 2), (a3, 0), (a2, 2), (a3, 1), (a4, 0), (a3, 2), (a4, 1), (a4, 2),
             (last, 0), (last, 1), (last, 2)]
    for fn, j in order:
        run(fn, j)
    nz.wait_send()

    def st_end(blk, _):
        for k in range(1, n_cls):
            st_copy(blk, k).wait_send()
        return 0

    lax.fori_loop(0, rows // 256, st_end, 0)


def local(features, labels, weight, noise):
    rows, depth = features.shape
    width = weight.shape[1]
    n_cls = lax.axis_size("cls")
    scale = 0.1 * (width * n_cls) / (rows * lax.axis_size("ex"))
    any_spec = pl.BlockSpec(memory_space=pl.ANY)
    vmem = pl.BlockSpec(memory_space=pltpu.VMEM)
    dma = pltpu.SemaphoreType.DMA
    blocks = rows // 256
    out = pl.pallas_call(
        functools.partial(kernel, scale),
        out_shape=jax.ShapeDtypeStruct((16, 104, width), BF16),
        in_specs=[any_spec, vmem, any_spec, any_spec],
        out_specs=vmem,
        scratch_shapes=[
            pltpu.VMEM((rows, depth), BF16),
            pltpu.VMEM((depth, width), BF16),
            pltpu.VMEM((depth, rows), BF16),
            pltpu.VMEM((rows, width), F32),
            pltpu.VMEM((6, rows, WIDE), BF16),
            pltpu.VMEM((rows, LANES), jnp.int32),
            pltpu.VMEM((LANES, LANES), F32),
            pltpu.VMEM((n_cls, blocks, 8, LANES), F32),
            pltpu.VMEM((blocks, 8, LANES), F32),
            pltpu.VMEM((3, depth, WIDE), F32),
            pltpu.VMEM((3, depth, WIDE), F32),
            pltpu.VMEM((3, 4, 4, 104, WIDE), BF16),
            pltpu.VMEM((3, 6, 2, 104, WIDE), BF16),
            pltpu.VMEM((3, 4, 104, WIDE), F32),
            pltpu.VMEM((3, 4, 104, WIDE), BF16),
            pltpu.VMEM((3, 6, 56, WIDE), BF16),
            pltpu.VMEM((6, 104, WIDE), F32),
            pltpu.VMEM((104, width), BF16),
            pltpu.VMEM((2, 52, width), BF16),
            dma((4,)), dma((blocks, n_cls - 1)), dma((blocks, n_cls - 1)), dma, dma,
            dma((3,)), dma((3,)), dma((3, 6)), dma((3, 6)), dma((3, 6)), dma((3, 6)),
            dma((3, 4)), dma((3, 4)), dma((3, 8)), dma((3, 8)), dma((3, 4)), dma((3, 4)),
            dma((3, 16)), dma((3, 16)),
        ],
        compiler_params=pltpu.CompilerParams(
            collective_id=0, has_side_effects=True, vmem_limit_bytes=67_043_328),
        cost_estimate=pl.CostEstimate(flops=4 * rows * depth * width, bytes_accessed=16_000_000, transcendentals=rows * width),
    )(features, labels.reshape(8, 128), weight, noise)
    return out.reshape(depth, width)


def solution(mesh):
    in_specs = (P("ex", None), P("ex"), P(None, "cls"), P("ex", "cls"))
    out_specs = P(None, "cls")
    return jax.shard_map(local, mesh=mesh, in_specs=in_specs, out_specs=out_specs, check_vma=False)
```

```python
import functools

import jax
import jax.numpy as jnp
from jax import lax
from jax.experimental import pallas as pl
from jax.experimental.pallas import tpu as pltpu
from jax.sharding import PartitionSpec as P

MESH = pl.DeviceIdType.MESH
F32, BF16 = jnp.float32, jnp.bfloat16
CLIP = 48.0
WIDE = 256
LANES = 128
ROWS = ((0, 48), (48, 56))

ORDER = " ".join((
    "part0 part1 own0 opp0", "ind0 opp1 own1 ind1", "opp3 part2 opp2 ind2",
    "r10 ind3 own2 opp4", "r11 r13 opp5 r12", "r20 ind4 r14 r21",
    "ind5 r23 r15 r30", "r22 r31 r24 r33", "u0 r32 r25 r34",
    "u1 u3 a10 u2", "r35 u4 a11 a12", "u5 a13 a21 a14",
    "a22 a15 a23 a20", "a31 a24 a25 a32", "a33 a30 a34 a35",
    "a43 a40 a41 a42", "a44 a45",
))


def kernel(scale, f_hbm, lab_hbm, w_hbm, noise_hbm, out_ref,
           f_v, w_v, ft_v, e_v, coef_v, lab_v, labrow_v, xt_v, st_v, fn_v, psend_v, precv_v,
           g_v, ra_v, hf_v, hs_v, rb_v, base_v, wown_v, nz_v,
           ld_sem, w_sem, f_sem, st_s, st_r, nz_s, nz_r, p_s, p_r, out_s, in_r):
    rows, depth = f_hbm.shape
    width = w_hbm.shape[1]
    tiles = width // LANES
    blocks = rows // WIDE
    n_cls = lax.axis_size("cls")
    ex = lax.axis_index("ex")
    z = lax.axis_index("cls")
    core = ex % 2
    c = 1 - core
    x = ex // 8
    y = (ex // 2) % 4
    a = x * (1 - c) + y * c
    b = y * (1 - c) + x * c

    def spot(i, j):
        return i * (4 - 3 * c) + j * (1 + 3 * c)

    def dev(i, j):
        return spot(i, j) * 2 + core

    mine = spot(a, b)
    a_up, a_dn, a_op = (a + 1) % 4, (a + 3) % 4, (a + 2) % 4
    b_up, b_dn, b_op = (b + 1) % 4, (b + 3) % 4, (b + 2) % 4
    to_aup, to_adn = dev(a_up, b), dev(a_dn, b)
    to_bup, to_bdn = dev(a, b_up), dev(a, b_dn)
    partner = ex + 1 - 2 * core

    w_tiles = [(n, min(WIDE, width - n)) for n in range(0, width, WIDE)]

    def f_load(i):
        r = pl.ds(i * WIDE, WIDE)
        return pltpu.make_async_copy(f_hbm.at[r, :], f_v.at[r, :], f_sem.at[i])

    w_load = pltpu.make_async_copy(w_hbm, w_v, w_sem)

    lab_load = pltpu.make_async_copy(lab_hbm, labrow_v, ld_sem.at[0])
    own_load = pltpu.make_async_copy(
        w_hbm.at[pl.ds(pl.multiple_of(mine * 104, 8), 104), :], wown_v, ld_sem.at[1])
    nz_load = pltpu.make_async_copy(noise_hbm, nz_v.at[core], ld_sem.at[2])
    lab_load.start()
    f_load(0).start()
    w_load.start()

    barrier = pltpu.get_barrier_semaphore()
    for t in (to_aup, to_adn, to_bup, to_bdn, partner):
        pl.semaphore_signal(barrier, inc=1, device_id={"ex": t}, device_id_type=MESH)
    for k in range(1, n_cls):
        pl.semaphore_signal(barrier, inc=1, device_id={"cls": (z + k) % n_cls}, device_id_type=MESH)

    def send(src, dst, s, r, t):
        return pltpu.make_async_remote_copy(
            src_ref=src, dst_ref=dst, send_sem=s, recv_sem=r, device_id={"ex": t}, device_id_type=MESH)

    coef_v[5, :, LANES:] = jnp.zeros((rows, LANES), BF16)
    lane = lax.broadcasted_iota(jnp.int32, (64, LANES), 1)

    def st_copy(blk, k):
        return pltpu.make_async_remote_copy(
            src_ref=st_v.at[z, blk], dst_ref=st_v.at[z, blk], send_sem=st_s, recv_sem=st_r.at[blk], device_id={"cls": (z + k) % n_cls}, device_id_type=MESH)

    def sums(blk, i):
        h, s = i // 2, i % 2
        r = slice(blk * WIDE + i * 64, blk * WIDE + (i + 1) * 64)
        top = e_v[r, 0:LANES]
        for n in range(1, tiles):
            top = jnp.maximum(top, e_v[r, n * LANES:(n + 1) * LANES])
        top = jnp.max(top, axis=1, keepdims=True)
        lab = lab_v[r, :]
        zero = jnp.zeros((64, LANES), F32)
        one, two, hit, sq = zero, zero, zero, zero
        for n in range(tiles):
            v = jnp.exp(e_v[r, n * LANES:(n + 1) * LANES] - top)
            e_v[r, n * LANES:(n + 1) * LANES] = v
            one += v
            two += v * v
            hit += jnp.where(lane + n * LANES == lab, v, 0.0)
        for k in range(depth // LANES):
            v = f_v[r, k * LANES:(k + 1) * LANES].astype(F32)
            sq += v * v
        one = jnp.sum(one, axis=1, keepdims=True)
        two = jnp.sum(two, axis=1, keepdims=True)
        hit = jnp.sum(hit, axis=1, keepdims=True)
        sq = jnp.sum(sq, axis=1, keepdims=True)
        pick = jnp.where(lane == 4 * h, top, 0.0)
        pick = jnp.where(lane == 4 * h + 1, one, pick)
        pick = jnp.where(lane == 4 * h + 2, two, pick)
        pick = jnp.where(lane == 4 * h + 3, hit, pick)
        pick = jnp.where(lane == 8 + h, sq, pick)
        if h == 0:
            xt_v[blk, s * 64:(s + 1) * 64, :] = pick
        else:
            xt_v[blk, s * 64:(s + 1) * 64, :] += pick

    def labels_of(blk):
        if blk == 0:
            lab_load.wait()
        for i in (2 * blk, 2 * blk + 1):
            row = jnp.broadcast_to(labrow_v[i:i + 1, :].astype(F32), (LANES, LANES))
            lab_v[i * LANES:(i + 1) * LANES, :] = row.T.astype(jnp.int32) - z * width

    def forward(blk):
        r = slice(blk * WIDE, (blk + 1) * WIDE)
        if blk < blocks:
            with jax.named_scope("load"):
                f_load(blk).wait()
            with jax.named_scope("labels"):
                labels_of(blk)
            if blk == 0:
                for i in range(1, blocks):
                    f_load(i).start()
                with jax.named_scope("wload"):
                    w_load.wait()
        for i, (n, w) in enumerate(w_tiles):
            if blk < blocks:
                e_v[r, n:n + w] = jnp.dot(f_v[r, :], w_v[:, n:n + w], preferred_element_type=F32)
            if blk > 0 and i < 4:
                sums(blk - 1, i)
        if blk == 0:
            own_load.start()
            nz_load.start()
        if blk == 1:
            pl.semaphore_wait(barrier, 5 + n_cls - 1)
        if blk > 0:
            t = xt_v[blk - 1].T
            st_v[z, blk - 1] = t[0:8]
            fn_v[blk - 1] = t[8:16]
            for k in range(1, n_cls):
                st_copy(blk - 1, k).start()

    for blk in range(blocks + 1):
        with jax.named_scope(f"forward_{blk}"):
            forward(blk)

    with jax.named_scope("turn"):
        nz = send(noise_hbm, nz_v.at[core], nz_s, nz_r, partner)
        nz.start()

        def turn(i, _):
            r = pl.ds(pl.multiple_of(i * LANES, LANES), LANES)
            ft_v[:, r] = f_v[r, :].T
            return 0

        lax.fori_loop(0, rows // LANES, turn, 0)

    def weigh(blk, _):
        ref = st_v.at[pl.ds(0, n_cls - 1), blk]
        send(ref, ref, st_s, st_r.at[blk], partner).wait_recv()
        for h in range(2):
            tops = [st_v[p, blk, 4 * h:4 * h + 1, :] for p in range(n_cls)]
            top = functools.reduce(jnp.maximum, tops)
            total = jnp.zeros((1, LANES), F32)
            squares, hit = total, total
            for p in range(n_cls):
                g = jnp.exp(tops[p] - top)
                total += st_v[p, blk, 4 * h + 1:4 * h + 2, :] * g
                squares += st_v[p, blk, 4 * h + 2:4 * h + 3, :] * (g * g)
                hit += st_v[p, blk, 4 * h + 3:4 * h + 4, :] * g
            prob = hit / total
            miss = 1.0 - prob
            resid = jnp.maximum(squares / (total * total) - prob * prob, 0.0) + miss * miss
            norm = jnp.sqrt(fn_v[blk, h:h + 1, :]) * jnp.sqrt(resid)
            factor = CLIP / jnp.maximum(norm, CLIP)
            up = factor * jnp.exp(st_v[z, blk, 4 * h:4 * h + 1, :] - top) / total
            up = jnp.broadcast_to(up, (LANES, LANES)).T
            down = jnp.broadcast_to(factor, (LANES, LANES)).T
            for s in range(2):
                r = pl.ds(pl.multiple_of(blk * WIDE + h * 128 + s * 64, 64), 64)
                lab = lab_v[r, :]
                u, d = up[s * 64:(s + 1) * 64], down[s * 64:(s + 1) * 64]
                for n in range(tiles):
                    v = e_v[r, n * LANES:(n + 1) * LANES] * u
                    v -= jnp.where(lane + n * LANES == lab, d, 0.0)
                    coef_v[n // 2, r, (n % 2) * LANES:(n % 2 + 1) * LANES] = v.astype(BF16)
        return 0

    with jax.named_scope("weigh012"):
        lax.fori_loop(0, blocks - 1, weigh, 0)
    with jax.named_scope("base"):
        own_load.wait()
        nz_load.wait()
        nz.wait_recv()
        for n in range(tiles):
            cols = slice(n * LANES, (n + 1) * LANES)
            base_v[n] = wown_v[:, cols].astype(F32)
            for i in range(2):
                base_v[n, i * 52:(i + 1) * 52] -= (scale * 0.96 * CLIP) * nz_v[i, :, cols].astype(F32)
    with jax.named_scope("weigh3"):
        weigh(blocks - 1, 0)

    half = depth // 2

    def p_send(k, i):
        r = pl.ds(pl.multiple_of(i * half, 16), half)
        return send(psend_v.at[k, r, :], precv_v.at[k, r, :], p_s, p_r.at[k, i], partner)

    def strip(i, m):
        return pl.ds(pl.multiple_of(i * half + m * 208, 16), 208)

    def part(k):
        def body(i, _):
            for m in range(4):
                psend_v[k, strip(i, m), :] = jnp.dot(
                    ft_v[strip(i, m), :], coef_v[(1 - c) * 3 + k], preferred_element_type=F32).astype(BF16)
            p_send(k, i).start()
            return 0
        lax.fori_loop(0, 2, body, 0)

    def own(k):
        def body(i, _):
            p_send(k, i).wait_recv()
            for m in range(4):
                acc = jnp.dot(ft_v[strip(i, m), :], coef_v[c * 3 + k], preferred_element_type=F32)
                acc += precv_v[k, strip(i, m), :].astype(F32)
                for n in range(2):
                    q = spot(2 * i + m // 2, 2 * (m % 2) + n)
                    for h in range(2):
                        g_v[2 * k + h, q // 4, q % 4] = acc[
                            n * 104:(n + 1) * 104, h * LANES:(h + 1) * LANES].astype(BF16)
            return 0
        lax.fori_loop(0, 2, body, 0)

    def arrived(ref, j, k):
        send(ref, ref, out_s.at[0], in_r.at[j, k], partner).wait_recv()

    def a_msg(j, k):
        group, hf, t = ((a_op, 0, to_aup), (a_op, 1, to_adn), (a_up, 1, to_aup),
                        (a_dn, 0, to_adn), (a_up, 0, to_aup), (a_dn, 1, to_adn))[k]
        return send(g_v.at[j, group, pl.ds(2 * hf, 2)], ra_v.at[j, k], out_s.at[0], in_r.at[j, 0 if k < 2 else 1], t)

    def b_msg(j, k):
        piece, hf, t = ((b_op, 0, to_bup), (b_op, 1, to_bdn), (b_up, 1, to_bup),
                        (b_dn, 0, to_bdn), (b_up, 0, to_bup), (b_dn, 1, to_bdn))[k]
        r0, nr = ROWS[hf]
        return send(hs_v.at[j, piece, pl.ds(r0, nr)], rb_v.at[j, k, pl.ds(0, nr)],
                    out_s.at[1], in_r.at[j, 2 if k < 2 else 3], t)

    def opp(j):
        a_msg(j, 0).start()
        a_msg(j, 1).start()

    def ind(j):
        a_msg(j, 2).start()
        a_msg(j, 3).start()

    def r1(j):
        arrived(ra_v.at[j, pl.ds(0, 2)], j, 0)
        for k, group, hf in ((0, a_up, 0), (1, a_dn, 1)):
            for i in range(2):
                v = g_v[j, group, 2 * hf + i].astype(F32) + ra_v[j, k, i].astype(F32)
                g_v[j, group, 2 * hf + i] = v.astype(BF16)
            a_msg(j, 4 + k).start()

    def r2(j):
        arrived(ra_v.at[j, pl.ds(2, 4)], j, 1)
        for hf, dep, alone in ((0, 4, 3), (1, 5, 2)):
            for i in range(2):
                v = g_v[j, a, 2 * hf + i].astype(F32) + ra_v[j, dep, i].astype(F32)
                v += ra_v[j, alone, i].astype(F32)
                hf_v[j, 2 * hf + i] = v
                hs_v[j, 2 * hf + i] = v.astype(BF16)
        for k in range(4):
            b_msg(j, k).start()

    def r3(j):
        arrived(hs_v.at[j, 0], j, 2)
        for k, piece, hf in ((0, b_up, 0), (1, b_dn, 1)):
            r0, nr = ROWS[hf]
            v = hf_v[j, piece, r0:r0 + nr] + rb_v[j, k, 0:nr].astype(F32)
            hs_v[j, piece, r0:r0 + nr] = v.astype(BF16)
            b_msg(j, 4 + k).start()

    def cols(j):
        return pl.ds(pl.multiple_of((c * 6 + j) * LANES, LANES), LANES)

    def place(j, p, hf=None):
        if hf is None:
            return out_ref.at[p, :, cols(j)]
        return out_ref.at[p, pl.ds(*ROWS[hf]), cols(j)]

    def g1(j, k):
        piece, hf, t = ((mine, None, to_bup), (mine, None, to_bdn),
                        (spot(a, b_dn), 0, to_bup), (spot(a, b_up), 1, to_bdn))[k]
        ref = place(j, piece, hf)
        return send(ref, ref, out_s.at[2], in_r.at[j, 4 if k < 2 else 5], t)

    near = (b, b_dn, b_up, b_op)

    def g2(j, r, up):
        ref = place(j, spot(a, near[r]))
        return send(ref, ref, out_s.at[3], in_r.at[j, 6 + r], to_aup if up else to_adn)

    def g3(j, r):
        ref = place(j, spot(a_dn if r < 2 else a_up, near[r]))
        return send(ref, ref, out_s.at[4], in_r.at[j, 10], to_aup if r < 2 else to_adn)

    def d2d(j, i, r):
        ref = place(j, spot((a, a_dn, a_up, a_op)[i], near[r]))
        return send(ref, ref, out_s.at[5], in_r.at[j, 11], partner)

    def have(j, r):
        g2(j, r, 1).start()
        g2(j, r, 0).start()
        d2d(j, 0, r).start()

    def u(j):
        arrived(hs_v.at[j, pl.ds(0, 2)], j, 3)
        for hf, dep, alone in ((0, 4, 3), (1, 5, 2)):
            r0, nr = ROWS[hf]
            v = hf_v[j, b, r0:r0 + nr] + rb_v[j, dep, 0:nr].astype(F32)
            v += rb_v[j, alone, 0:nr].astype(F32)
            v = base_v[c * 6 + j, r0:r0 + nr] - scale * v
            out_ref[mine, r0:r0 + nr, cols(j)] = v.astype(BF16)
        g1(j, 0).start()
        g1(j, 1).start()
        have(j, 0)

    def a1(j):
        arrived(hs_v.at[j, pl.ds(0, 2)], j, 4)
        g1(j, 2).start()
        g1(j, 3).start()
        have(j, 1)
        have(j, 2)

    def a2(j):
        arrived(hs_v.at[j, 0], j, 5)
        have(j, 3)

    def a3(j):
        for r in range(4):
            arrived(hs_v.at[j, pl.ds(0, 2)], j, 6 + r)
            g3(j, r).start()
            d2d(j, 1, r).start()
            d2d(j, 2, r).start()

    def a4(j):
        arrived(hs_v.at[j], j, 10)
        for r in range(4):
            d2d(j, 3, r).start()

    def run(fn, j, role=0):
        with jax.named_scope(f"{fn.__name__}_{j}"):
            if j < 5:
                fn(j)
            else:
                pl.when(c == role)(lambda: fn(j))

    stages = dict(part=part, own=own, opp=opp, ind=ind, r1=r1, r2=r2, r3=r3, u=u, a1=a1, a2=a2, a3=a3, a4=a4)
    for word in ORDER.split():
        name, j = word[:-1], int(word[-1])
        if name in ("part", "own"):
            with jax.named_scope(word):
                stages[name](j)
        else:
            run(stages[name], j)

    def drain(n):
        for k, ref in enumerate((ra_v.at[pl.ds(0, n)], hs_v.at[pl.ds(0, n), pl.ds(0, 3)], hs_v.at[pl.ds(0, n), pl.ds(0, 3)],
                                 g_v.at[pl.ds(0, n), pl.ds(0, 2)], hs_v.at[pl.ds(0, n)], g_v.at[pl.ds(0, n)])):
            send(ref, ref, out_s.at[k], in_r.at[0, 0], partner).wait_send()

    with jax.named_scope("partner"):
        for j in range(6):
            run(lambda k: arrived(g_v.at[k], k, 11), j, 1)
    with jax.named_scope("drain"):
        pl.when(c == 0)(lambda: drain(6))
        pl.when(c == 1)(lambda: drain(5))
    nz.wait_send()
    send(psend_v, precv_v, p_s, p_r.at[0, 0], partner).wait_send()
    ref = st_v.at[pl.ds(0, n_cls - 1)]
    send(ref, ref, st_s, st_r.at[0], partner).wait_send()


def local(features, labels, weight, noise):
    rows, depth = features.shape
    width = weight.shape[1]
    n_cls = lax.axis_size("cls")
    scale = 0.1 * (width * n_cls) / (rows * lax.axis_size("ex"))
    hbm = pl.BlockSpec(memory_space=pltpu.HBM)
    dma = pltpu.SemaphoreType.DMA
    blocks = rows // WIDE
    args = [pltpu.with_memory_space_constraint(v, pltpu.HBM)
            for v in (features, labels.reshape(rows // LANES, LANES), weight, noise)]
    out = pl.pallas_call(
        functools.partial(kernel, scale),
        out_shape=jax.ShapeDtypeStruct((16, 104, width), BF16),
        in_specs=[hbm] * 4,
        out_specs=pl.BlockSpec(memory_space=pltpu.VMEM),
        scratch_shapes=[
            pltpu.VMEM((rows, depth), BF16),
            pltpu.VMEM((depth, width), BF16),
            pltpu.VMEM((depth, rows), BF16),
            pltpu.VMEM((rows, width), F32),
            pltpu.VMEM((6, rows, WIDE), BF16),
            pltpu.VMEM((rows, LANES), jnp.int32),
            pltpu.VMEM((rows // LANES, LANES), jnp.int32),
            pltpu.VMEM((blocks, LANES, LANES), F32),
            pltpu.VMEM((n_cls, blocks, 8, LANES), F32),
            pltpu.VMEM((blocks, 8, LANES), F32),
            pltpu.VMEM((3, depth, WIDE), BF16),
            pltpu.VMEM((3, depth, WIDE), BF16),
            pltpu.VMEM((6, 4, 4, 104, LANES), BF16),
            pltpu.VMEM((6, 6, 2, 104, LANES), BF16),
            pltpu.VMEM((6, 4, 104, LANES), F32),
            pltpu.VMEM((6, 4, 104, LANES), BF16),
            pltpu.VMEM((6, 6, 56, LANES), BF16),
            pltpu.VMEM((width // LANES, 104, LANES), F32),
            pltpu.VMEM((104, width), BF16),
            pltpu.VMEM((2, 52, width), BF16),
            dma((3,)), dma, dma((blocks,)), dma, dma((blocks,)), dma, dma,
            dma, dma((3, 2)), dma((6,)), dma((6, 12)),
        ],
        compiler_params=pltpu.CompilerParams(
            collective_id=0, has_side_effects=True, vmem_limit_bytes=48_000_000),
        cost_estimate=pl.CostEstimate(flops=4 * rows * depth * width, bytes_accessed=16_000_000,
                                      transcendentals=rows * width),
    )(*args)
    return out.reshape(depth, width)


def solution(mesh):
    in_specs = (P("ex", None), P("ex"), P(None, "cls"), P("ex", "cls"))
    out_specs = P(None, "cls")
    return jax.shard_map(local, mesh=mesh, in_specs=in_specs, out_specs=out_specs, check_vma=False)
```

```python
import functools

import jax
import jax.numpy as jnp
from jax import lax
from jax.experimental import pallas as pl
from jax.experimental.pallas import tpu as pltpu
from jax.sharding import PartitionSpec as P

MESH = pl.DeviceIdType.MESH
F32, BF16 = jnp.float32, jnp.bfloat16
CLIP = 48.0
WIDE = 256
LANES = 128
ROWS = ((0, 48), (48, 56))

ORDER = " ".join((
    "part0 part1 own0 opp1", "opp0 ind1 ind0 own1", "opp2 opp3 part2 ind3",
    "r11 r10 ind2 own2", "opp4 r12 r13 r21", "opp5 r20 r30 ind4",
    "r14 r22 r23 r31", "r15 ind5 u1 r33", "u0 r32 r24 u3",
    "r25 r34 a11 a10", "u2 r35 u5 u4", "a13 a21 a23 a12",
    "a22 a20 a15 a14", "a24 a25 a31 a33", "a32 a30 a34 a35",
    "a40 a43 a41 a42", "a45 a44",
))
FAR_RS_A = ()
FAR_RS_B = (0, 1, 3, 4, 5)
FAR_AG_B = (2, 3, 4, 5)
FAR_AG_A = ()


def kernel(scale, f_hbm, lab_hbm, w_hbm, noise_hbm, out_ref,
           f_v, w_v, ft_v, e_v, coef_v, lab_v, labrow_v, xt_v, st_v, fn_v, psend_v, precv_v,
           g_v, ra_v, hf_v, hs_v, rb_v, rf_v, base_v, wown_v, nz_v,
           ld_sem, w_sem, f_sem, st_s, st_r, nz_s, nz_r, p_s, p_r, out_s, in_r):
    rows, depth = f_hbm.shape
    width = w_hbm.shape[1]
    tiles = width // LANES
    blocks = rows // WIDE
    n_cls = lax.axis_size("cls")
    ex = lax.axis_index("ex")
    z = lax.axis_index("cls")
    core = ex % 2
    c = 1 - core
    x = ex // 8
    y = (ex // 2) % 4
    a = x * (1 - c) + y * c
    b = y * (1 - c) + x * c

    def spot(i, j):
        return i * (4 - 3 * c) + j * (1 + 3 * c)

    def dev(i, j):
        return spot(i, j) * 2 + core

    mine = spot(a, b)
    a_up, a_dn, a_op = (a + 1) % 4, (a + 3) % 4, (a + 2) % 4
    b_up, b_dn, b_op = (b + 1) % 4, (b + 3) % 4, (b + 2) % 4
    to_aup, to_adn = dev(a_up, b), dev(a_dn, b)
    to_bup, to_bdn = dev(a, b_up), dev(a, b_dn)
    to_aop, to_bop = dev(a_op, b), dev(a, b_op)
    partner = ex + 1 - 2 * core

    w_tiles = [(n, min(WIDE, width - n)) for n in range(0, width, WIDE)]

    def f_load(i):
        r = pl.ds(i * WIDE, WIDE)
        return pltpu.make_async_copy(f_hbm.at[r, :], f_v.at[r, :], f_sem.at[i])

    parts = ((0, 768), (768, depth - 768))

    def w_load(i):
        r = pl.ds(*parts[i])
        return pltpu.make_async_copy(w_hbm.at[r, :], w_v.at[r, :], w_sem.at[i])

    lab_load = pltpu.make_async_copy(lab_hbm, labrow_v, ld_sem.at[0])
    own_load = pltpu.make_async_copy(
        w_hbm.at[pl.ds(pl.multiple_of(mine * 104, 8), 104), :], wown_v, ld_sem.at[1])
    nz_load = pltpu.make_async_copy(noise_hbm, nz_v.at[core], ld_sem.at[2])
    lab_load.start()
    f_load(0).start()
    w_load(0).start()
    w_load(1).start()

    barrier = pltpu.get_barrier_semaphore()
    for t in (to_aup, to_adn, to_aop, to_bup, to_bdn, to_bop, partner):
        pl.semaphore_signal(barrier, inc=1, device_id={"ex": t}, device_id_type=MESH)
    for k in range(1, n_cls):
        pl.semaphore_signal(barrier, inc=1, device_id={"cls": (z + k) % n_cls}, device_id_type=MESH)

    def send(src, dst, s, r, t):
        return pltpu.make_async_remote_copy(
            src_ref=src, dst_ref=dst, send_sem=s, recv_sem=r, device_id={"ex": t}, device_id_type=MESH)

    coef_v[5, :, LANES:] = jnp.zeros((rows, LANES), BF16)
    lane = lax.broadcasted_iota(jnp.int32, (64, LANES), 1)

    def st_copy(blk, k):
        return pltpu.make_async_remote_copy(
            src_ref=st_v.at[z, blk], dst_ref=st_v.at[z, blk], send_sem=st_s, recv_sem=st_r.at[blk], device_id={"cls": (z + k) % n_cls}, device_id_type=MESH)

    def sums(blk, i):
        h, s = i // 2, i % 2
        r = slice(blk * WIDE + i * 64, blk * WIDE + (i + 1) * 64)
        top = e_v[r, 0:LANES]
        for n in range(1, tiles):
            top = jnp.maximum(top, e_v[r, n * LANES:(n + 1) * LANES])
        top = jnp.max(top, axis=1, keepdims=True)
        lab = lab_v[r, :]
        zero = jnp.zeros((64, LANES), F32)
        one, two, hit, sq = zero, zero, zero, zero
        for n in range(tiles):
            v = jnp.exp(e_v[r, n * LANES:(n + 1) * LANES] - top)
            e_v[r, n * LANES:(n + 1) * LANES] = v
            one += v
            two += v * v
            hit += jnp.where(lane + n * LANES == lab, v, 0.0)
        for k in range(depth // LANES):
            v = f_v[r, k * LANES:(k + 1) * LANES].astype(F32)
            sq += v * v
        one = jnp.sum(one, axis=1, keepdims=True)
        two = jnp.sum(two, axis=1, keepdims=True)
        hit = jnp.sum(hit, axis=1, keepdims=True)
        sq = jnp.sum(sq, axis=1, keepdims=True)
        pick = jnp.where(lane == 4 * h, top, 0.0)
        pick = jnp.where(lane == 4 * h + 1, one, pick)
        pick = jnp.where(lane == 4 * h + 2, two, pick)
        pick = jnp.where(lane == 4 * h + 3, hit, pick)
        pick = jnp.where(lane == 8 + h, sq, pick)
        if h == 0:
            xt_v[blk, s * 64:(s + 1) * 64, :] = pick
        else:
            xt_v[blk, s * 64:(s + 1) * 64, :] += pick

    def labels_of(blk):
        if blk == 0:
            lab_load.wait()
        for i in (2 * blk, 2 * blk + 1):
            row = jnp.broadcast_to(labrow_v[i:i + 1, :].astype(F32), (LANES, LANES))
            lab_v[i * LANES:(i + 1) * LANES, :] = row.T.astype(jnp.int32) - z * width

    def turn(i):
        ft_v[:, i * LANES:(i + 1) * LANES] = f_v[i * LANES:(i + 1) * LANES, :].T

    def forward(blk):
        r = slice(blk * WIDE, (blk + 1) * WIDE)
        if blk < blocks:
            with jax.named_scope("load"):
                f_load(blk).wait()
            with jax.named_scope("labels"):
                labels_of(blk)
        if blk == 0:
            for i in range(1, blocks):
                f_load(i).start()
            for i, (k, nk) in enumerate(parts):
                w_load(i).wait()
                for n, w in w_tiles:
                    v = jnp.dot(f_v[r, k:k + nk], w_v[k:k + nk, n:n + w], preferred_element_type=F32)
                    e_v[r, n:n + w] = v if i == 0 else v + e_v[r, n:n + w]
        for i, (n, w) in enumerate(w_tiles):
            if 0 < blk < blocks:
                e_v[r, n:n + w] = jnp.dot(f_v[r, :], w_v[:, n:n + w], preferred_element_type=F32)
            if blk > 0 and i < 4:
                sums(blk - 1, i)
            if 0 < blk < blocks and i >= 4:
                turn((blk - 1) * 2 + i - 4)
        if blk == 0:
            own_load.start()
            nz_load.start()
        if blk == 1:
            pl.semaphore_wait(barrier, 7 + n_cls - 1)
        if blk > 0:
            t = xt_v[blk - 1].T
            st_v[z, blk - 1] = t[0:8]
            fn_v[blk - 1] = t[8:16]
            for k in range(1, n_cls):
                st_copy(blk - 1, k).start()

    for blk in range(blocks + 1):
        with jax.named_scope(f"forward_{blk}"):
            forward(blk)

    with jax.named_scope("turn"):
        nz = send(noise_hbm, nz_v.at[core], nz_s, nz_r, partner)
        nz.start()

        for i in (2 * blocks - 2, 2 * blocks - 1):
            turn(i)

    def weigh(blk, _):
        ref = st_v.at[pl.ds(0, n_cls - 1), blk]
        send(ref, ref, st_s, st_r.at[blk], partner).wait_recv()
        for h in range(2):
            tops = [st_v[p, blk, 4 * h:4 * h + 1, :] for p in range(n_cls)]
            top = functools.reduce(jnp.maximum, tops)
            total = jnp.zeros((1, LANES), F32)
            squares, hit = total, total
            for p in range(n_cls):
                g = jnp.exp(tops[p] - top)
                total += st_v[p, blk, 4 * h + 1:4 * h + 2, :] * g
                squares += st_v[p, blk, 4 * h + 2:4 * h + 3, :] * (g * g)
                hit += st_v[p, blk, 4 * h + 3:4 * h + 4, :] * g
            prob = hit / total
            miss = 1.0 - prob
            resid = jnp.maximum(squares / (total * total) - prob * prob, 0.0) + miss * miss
            norm = jnp.sqrt(fn_v[blk, h:h + 1, :]) * jnp.sqrt(resid)
            factor = CLIP / jnp.maximum(norm, CLIP)
            up = factor * jnp.exp(st_v[z, blk, 4 * h:4 * h + 1, :] - top) / total
            up = jnp.broadcast_to(up, (LANES, LANES)).T
            down = jnp.broadcast_to(factor, (LANES, LANES)).T
            for s in range(2):
                r = pl.ds(pl.multiple_of(blk * WIDE + h * 128 + s * 64, 64), 64)
                lab = lab_v[r, :]
                u, d = up[s * 64:(s + 1) * 64], down[s * 64:(s + 1) * 64]
                for n in range(tiles):
                    v = e_v[r, n * LANES:(n + 1) * LANES] * u
                    v -= jnp.where(lane + n * LANES == lab, d, 0.0)
                    coef_v[n // 2, r, (n % 2) * LANES:(n % 2 + 1) * LANES] = v.astype(BF16)
        return 0

    with jax.named_scope("weigh012"):
        lax.fori_loop(0, blocks - 1, weigh, 0)
    with jax.named_scope("base"):
        own_load.wait()
        nz_load.wait()
        nz.wait_recv()
        for n in range(tiles):
            cols = slice(n * LANES, (n + 1) * LANES)
            base_v[n] = wown_v[:, cols].astype(F32)
            for i in range(2):
                base_v[n, i * 52:(i + 1) * 52] -= (scale * 0.96 * CLIP) * nz_v[i, :, cols].astype(F32)
    with jax.named_scope("weigh3"):
        weigh(blocks - 1, 0)

    half = depth // 2

    def p_send(k, i):
        r = pl.ds(pl.multiple_of(i * half, 16), half)
        return send(psend_v.at[k, r, :], precv_v.at[k, r, :], p_s, p_r.at[k, i], partner)

    def strip(i, m):
        return pl.ds(pl.multiple_of(i * half + m * 208, 16), 208)

    def part(k):
        def body(i, _):
            for m in range(4):
                psend_v[k, strip(i, m), :] = jnp.dot(
                    ft_v[strip(i, m), :], coef_v[(1 - c) * 3 + k], preferred_element_type=F32).astype(BF16)
            p_send(k, i).start()
            return 0
        lax.fori_loop(0, 2, body, 0)

    def own(k):
        def body(i, _):
            p_send(k, i).wait_recv()
            for m in range(4):
                acc = jnp.dot(ft_v[strip(i, m), :], coef_v[c * 3 + k], preferred_element_type=F32)
                acc += precv_v[k, strip(i, m), :].astype(F32)
                for n in range(2):
                    q = spot(2 * i + m // 2, 2 * (m % 2) + n)
                    for h in range(2):
                        g_v[2 * k + h, q // 4, q % 4] = acc[
                            n * 104:(n + 1) * 104, h * LANES:(h + 1) * LANES].astype(BF16)
            return 0
        lax.fori_loop(0, 2, body, 0)

    def arrived(ref, j, k):
        send(ref, ref, out_s.at[0], in_r.at[j, k], partner).wait_recv()

    def a_msg(j, k):
        group, hf, t = ((a_op, 0, to_aup), (a_op, 1, to_adn), (a_up, 1, to_aup),
                        (a_dn, 0, to_adn), (a_up, 0, to_aup), (a_dn, 1, to_adn))[k]
        return send(g_v.at[j, group, pl.ds(2 * hf, 2)], ra_v.at[j, pl.ds(2 * k, 2)], out_s.at[0], in_r.at[j, 0 if k < 2 else 1], t)

    def a_far(j, k):
        group, t = ((a_op, to_aop), (a_up, to_aup), (a_dn, to_adn))[k]
        return send(g_v.at[j, group], ra_v.at[j, pl.ds(4 * k, 4)], out_s.at[0], in_r.at[j, min(k, 1)], t)

    def b_far(j, k):
        piece, t = ((b_op, to_bop), (b_up, to_bup), (b_dn, to_bdn))[k]
        return send(hs_v.at[j, piece], rf_v.at[j, k], out_s.at[1], in_r.at[j, 2 + min(k, 1)], t)

    def b_msg(j, k):
        piece, hf, t = ((b_op, 0, to_bup), (b_op, 1, to_bdn), (b_up, 1, to_bup),
                        (b_dn, 0, to_bdn), (b_up, 0, to_bup), (b_dn, 1, to_bdn))[k]
        r0, nr = ROWS[hf]
        return send(hs_v.at[j, piece, pl.ds(r0, nr)], rb_v.at[j, k, pl.ds(0, nr)],
                    out_s.at[1], in_r.at[j, 2 if k < 2 else 3], t)

    def opp(j):
        if j in FAR_RS_A:
            a_far(j, 0).start()
            return
        a_msg(j, 0).start()
        a_msg(j, 1).start()

    def ind(j):
        if j in FAR_RS_A:
            a_far(j, 1).start()
            a_far(j, 2).start()
            return
        a_msg(j, 2).start()
        a_msg(j, 3).start()

    def r1(j):
        if j in FAR_RS_A:
            return
        arrived(ra_v.at[j, pl.ds(0, 4)], j, 0)
        for k, group, hf in ((0, a_up, 0), (1, a_dn, 1)):
            for i in range(2):
                v = g_v[j, group, 2 * hf + i].astype(F32) + ra_v[j, 2 * k + i].astype(F32)
                g_v[j, group, 2 * hf + i] = v.astype(BF16)
            a_msg(j, 4 + k).start()

    def r2(j):
        if j in FAR_RS_A:
            arrived(ra_v.at[j, pl.ds(0, 4)], j, 0)
        arrived(ra_v.at[j, pl.ds(4, 8)], j, 1)
        for i in range(4):
            v = g_v[j, a, i].astype(F32)
            for k in (i, 4 + i, 8 + i) if j in FAR_RS_A else ((8 + i, 6 + i) if i < 2 else (8 + i, 2 + i)):
                v += ra_v[j, k].astype(F32)
            hf_v[j, i] = v
            hs_v[j, i] = v.astype(BF16)
        for k in range(3 if j in FAR_RS_B else 4):
            (b_far if j in FAR_RS_B else b_msg)(j, k).start()

    def r3(j):
        if j in FAR_RS_B:
            return
        arrived(hs_v.at[j, 0], j, 2)
        for k, piece, hf in ((0, b_up, 0), (1, b_dn, 1)):
            r0, nr = ROWS[hf]
            v = hf_v[j, piece, r0:r0 + nr] + rb_v[j, k, 0:nr].astype(F32)
            hs_v[j, piece, r0:r0 + nr] = v.astype(BF16)
            b_msg(j, 4 + k).start()

    def cols(j):
        return pl.ds(pl.multiple_of((c * 6 + j) * LANES, LANES), LANES)

    def place(j, p, hf=None):
        if hf is None:
            return out_ref.at[p, :, cols(j)]
        return out_ref.at[p, pl.ds(*ROWS[hf]), cols(j)]

    def g1(j, k):
        piece, hf, t = ((mine, None, to_bup), (mine, None, to_bdn),
                        (spot(a, b_dn), 0, to_bup), (spot(a, b_up), 1, to_bdn))[k]
        ref = place(j, piece, hf)
        return send(ref, ref, out_s.at[2], in_r.at[j, 4 if k < 2 else 5], t)

    near = (b, b_dn, b_up, b_op)

    def g2(j, r, up):
        ref = place(j, spot(a, near[r]))
        return send(ref, ref, out_s.at[3], in_r.at[j, 6 + r], to_aup if up else to_adn)

    def g3(j, r):
        ref = place(j, spot(a_dn if r < 2 else a_up, near[r]))
        return send(ref, ref, out_s.at[4], in_r.at[j, 10], to_aup if r < 2 else to_adn)

    def d2d(j, i, r):
        ref = place(j, spot((a, a_dn, a_up, a_op)[i], near[r]))
        return send(ref, ref, out_s.at[5], in_r.at[j, 11], partner)

    def have(j, r):
        g2(j, r, 1).start()
        g2(j, r, 0).start()
        if j in FAR_AG_A:
            ref = place(j, spot(a, near[r]))
            send(ref, ref, out_s.at[4], in_r.at[j, 10], to_aop).start()
        d2d(j, 0, r).start()

    def u(j):
        if j in FAR_RS_B:
            arrived(hs_v.at[j, 0], j, 2)
        arrived(hs_v.at[j, pl.ds(0, 2)], j, 3)
        for hf, dep, alone in ((0, 4, 3), (1, 5, 2)):
            r0, nr = ROWS[hf]
            v = hf_v[j, b, r0:r0 + nr]
            if j in FAR_RS_B:
                for k in range(3):
                    v += rf_v[j, k, r0:r0 + nr].astype(F32)
            else:
                v += rb_v[j, dep, 0:nr].astype(F32)
                v += rb_v[j, alone, 0:nr].astype(F32)
            v = base_v[c * 6 + j, r0:r0 + nr] - scale * v
            out_ref[mine, r0:r0 + nr, cols(j)] = v.astype(BF16)
        g1(j, 0).start()
        g1(j, 1).start()
        if j in FAR_AG_B:
            ref = place(j, mine)
            send(ref, ref, out_s.at[2], in_r.at[j, 5], to_bop).start()
        have(j, 0)

    def a1(j):
        arrived(hs_v.at[j, pl.ds(0, 2)], j, 4)
        if j not in FAR_AG_B:
            g1(j, 2).start()
            g1(j, 3).start()
        have(j, 1)
        have(j, 2)

    def a2(j):
        arrived(hs_v.at[j, 0], j, 5)
        have(j, 3)

    def a3(j):
        for r in range(4):
            arrived(hs_v.at[j, pl.ds(0, 2)], j, 6 + r)
            if j not in FAR_AG_A:
                g3(j, r).start()
            d2d(j, 1, r).start()
            d2d(j, 2, r).start()

    def a4(j):
        arrived(hs_v.at[j], j, 10)
        for r in range(4):
            d2d(j, 3, r).start()

    def run(fn, j, role=0):
        with jax.named_scope(f"{fn.__name__}_{j}"):
            if j < 5:
                fn(j)
            else:
                pl.when(c == role)(lambda: fn(j))

    stages = dict(part=part, own=own, opp=opp, ind=ind, r1=r1, r2=r2, r3=r3, u=u, a1=a1, a2=a2, a3=a3, a4=a4)
    for word in ORDER.split():
        name, j = word[:-1], int(word[-1])
        if name in ("part", "own"):
            with jax.named_scope(word):
                stages[name](j)
        else:
            run(stages[name], j)

    def drain(n):
        for k, ref in enumerate((ra_v.at[pl.ds(0, n)], hs_v.at[pl.ds(0, n), pl.ds(0, 3)], hs_v.at[pl.ds(0, n), pl.ds(0, 3)],
                                 g_v.at[pl.ds(0, n), pl.ds(0, 2)], hs_v.at[pl.ds(0, n)], g_v.at[pl.ds(0, n)])):
            send(ref, ref, out_s.at[k], in_r.at[0, 0], partner).wait_send()

    with jax.named_scope("partner"):
        for j in range(6):
            run(lambda k: arrived(g_v.at[k], k, 11), j, 1)
    with jax.named_scope("drain"):
        pl.when(c == 0)(lambda: drain(6))
        pl.when(c == 1)(lambda: drain(5))
    nz.wait_send()
    send(psend_v, precv_v, p_s, p_r.at[0, 0], partner).wait_send()
    ref = st_v.at[pl.ds(0, n_cls - 1)]
    send(ref, ref, st_s, st_r.at[0], partner).wait_send()


def local(features, labels, weight, noise):
    rows, depth = features.shape
    width = weight.shape[1]
    n_cls = lax.axis_size("cls")
    scale = 0.1 * (width * n_cls) / (rows * lax.axis_size("ex"))
    hbm = pl.BlockSpec(memory_space=pltpu.HBM)
    dma = pltpu.SemaphoreType.DMA
    blocks = rows // WIDE
    args = [pltpu.with_memory_space_constraint(v, pltpu.HBM)
            for v in (features, labels.reshape(rows // LANES, LANES), weight, noise)]
    out = pl.pallas_call(
        functools.partial(kernel, scale),
        out_shape=jax.ShapeDtypeStruct((16, 104, width), BF16),
        in_specs=[hbm] * 4,
        out_specs=pl.BlockSpec(memory_space=pltpu.VMEM),
        scratch_shapes=[
            pltpu.VMEM((rows, depth), BF16),
            pltpu.VMEM((depth, width), BF16),
            pltpu.VMEM((depth, rows), BF16),
            pltpu.VMEM((rows, width), F32),
            pltpu.VMEM((6, rows, WIDE), BF16),
            pltpu.VMEM((rows, LANES), jnp.int32),
            pltpu.VMEM((rows // LANES, LANES), jnp.int32),
            pltpu.VMEM((blocks, LANES, LANES), F32),
            pltpu.VMEM((n_cls, blocks, 8, LANES), F32),
            pltpu.VMEM((blocks, 8, LANES), F32),
            pltpu.VMEM((3, depth, WIDE), BF16),
            pltpu.VMEM((3, depth, WIDE), BF16),
            pltpu.VMEM((6, 4, 4, 104, LANES), BF16),
            pltpu.VMEM((6, 12, 104, LANES), BF16),
            pltpu.VMEM((6, 4, 104, LANES), F32),
            pltpu.VMEM((6, 4, 104, LANES), BF16),
            pltpu.VMEM((6, 6, 56, LANES), BF16),
            pltpu.VMEM((6, 3, 104, LANES), BF16),
            pltpu.VMEM((width // LANES, 104, LANES), F32),
            pltpu.VMEM((104, width), BF16),
            pltpu.VMEM((2, 52, width), BF16),
            dma((3,)), dma((2,)), dma((blocks,)), dma, dma((blocks,)), dma, dma,
            dma, dma((3, 2)), dma((6,)), dma((6, 12)),
        ],
        compiler_params=pltpu.CompilerParams(
            collective_id=0, has_side_effects=True, vmem_limit_bytes=48_000_000),
        cost_estimate=pl.CostEstimate(flops=4 * rows * depth * width, bytes_accessed=16_000_000,
                                      transcendentals=rows * width),
    )(*args)
    return out.reshape(depth, width)


def solution(mesh):
    in_specs = (P("ex", None), P("ex"), P(None, "cls"), P("ex", "cls"))
    out_specs = P(None, "cls")
    return jax.shard_map(local, mesh=mesh, in_specs=in_specs, out_specs=out_specs, check_vma=False)
```

```python
import functools

import jax
import jax.numpy as jnp
from jax import lax
from jax.experimental import pallas as pl
from jax.experimental.pallas import tpu as pltpu
from jax.sharding import PartitionSpec as P

MESH = pl.DeviceIdType.MESH
F32, BF16 = jnp.float32, jnp.bfloat16
CLIP = 48.0
WIDE = 256
LANES = 128
ROWS = ((0, 48), (48, 56))

ORDER = " ".join((
    "part0 part1 own0 opp1", "opp0 ind1 ind0 own1", "opp2 opp3 part2 ind3",
    "r11 r10 ind2 own2", "opp4 r12 r13 r21", "opp5 r20 r30 ind4",
    "r14 r22 r23 r31", "r15 ind5 u1 r33", "u0 r32 r24 u3",
    "r25 r34 a11 a10", "u2 r35 u5 u4", "a13 a21 a23 a12",
    "a22 a20 a15 a14", "a24 a25 a31 a33", "a32 a30 a34 a35",
    "a40 a43 a41 a42", "a45 a44",
))
FAR_RS_A = ()
FAR_RS_B = (0, 1, 3, 4, 5)
FAR_AG_B = (2, 3, 4, 5)
FAR_AG_A = ()


def kernel(scale, f_hbm, lab_hbm, w_hbm, noise_hbm, out_ref,
           f_v, w_v, ft_v, e_v, coef_v, lab_v, labrow_v, xt_v, st_v, fn_v, psend_v, precv_v, acc_v,
           g_v, ra_v, hf_v, hs_v, rb_v, rf_v, base_v, wown_v, nz_v,
           ld_sem, w_sem, f_sem, st_s, st_r, nz_s, nz_r, p_s, p_r, out_s, in_r):
    rows, depth = f_hbm.shape
    width = w_hbm.shape[1]
    tiles = width // LANES
    blocks = rows // WIDE
    n_cls = lax.axis_size("cls")
    ex = lax.axis_index("ex")
    z = lax.axis_index("cls")
    core = ex % 2
    c = 1 - core
    x = ex // 8
    y = (ex // 2) % 4
    a = x * (1 - c) + y * c
    b = y * (1 - c) + x * c

    def spot(i, j):
        return i * (4 - 3 * c) + j * (1 + 3 * c)

    def dev(i, j):
        return spot(i, j) * 2 + core

    mine = spot(a, b)
    a_up, a_dn, a_op = (a + 1) % 4, (a + 3) % 4, (a + 2) % 4
    b_up, b_dn, b_op = (b + 1) % 4, (b + 3) % 4, (b + 2) % 4
    to_aup, to_adn = dev(a_up, b), dev(a_dn, b)
    to_bup, to_bdn = dev(a, b_up), dev(a, b_dn)
    to_aop, to_bop = dev(a_op, b), dev(a, b_op)
    partner = ex + 1 - 2 * core

    w_tiles = [(n, min(WIDE, width - n)) for n in range(0, width, WIDE)]

    def f_load(i):
        r = pl.ds(i * WIDE, WIDE)
        return pltpu.make_async_copy(f_hbm.at[r, :], f_v.at[r, :], f_sem.at[i])

    parts = ((0, 768), (768, depth - 768))

    def w_load(i):
        r = pl.ds(*parts[i])
        return pltpu.make_async_copy(w_hbm.at[r, :], w_v.at[r, :], w_sem.at[i])

    lab_load = pltpu.make_async_copy(lab_hbm, labrow_v, ld_sem.at[0])
    own_load = pltpu.make_async_copy(
        w_hbm.at[pl.ds(pl.multiple_of(mine * 104, 8), 104), :], wown_v, ld_sem.at[1])
    nz_load = pltpu.make_async_copy(noise_hbm, nz_v.at[core], ld_sem.at[2])
    lab_load.start()
    f_load(0).start()
    w_load(0).start()
    w_load(1).start()

    barrier = pltpu.get_barrier_semaphore()
    for t in (to_aup, to_adn, to_aop, to_bup, to_bdn, to_bop, partner):
        pl.semaphore_signal(barrier, inc=1, device_id={"ex": t}, device_id_type=MESH)
    for k in range(1, n_cls):
        pl.semaphore_signal(barrier, inc=1, device_id={"cls": (z + k) % n_cls}, device_id_type=MESH)

    def send(src, dst, s, r, t):
        return pltpu.make_async_remote_copy(
            src_ref=src, dst_ref=dst, send_sem=s, recv_sem=r, device_id={"ex": t}, device_id_type=MESH)

    coef_v[5, :, LANES:] = jnp.zeros((rows, LANES), BF16)
    lane = lax.broadcasted_iota(jnp.int32, (64, LANES), 1)

    def st_copy(blk, k):
        return pltpu.make_async_remote_copy(
            src_ref=st_v.at[z, blk], dst_ref=st_v.at[z, blk], send_sem=st_s, recv_sem=st_r.at[blk], device_id={"cls": (z + k) % n_cls}, device_id_type=MESH)

    def sums(blk, i):
        h, s = i // 2, i % 2
        r = slice(blk * WIDE + i * 64, blk * WIDE + (i + 1) * 64)
        top = e_v[r, 0:LANES]
        for n in range(1, tiles):
            top = jnp.maximum(top, e_v[r, n * LANES:(n + 1) * LANES])
        top = jnp.max(top, axis=1, keepdims=True)
        lab = lab_v[r, :]
        zero = jnp.zeros((64, LANES), F32)
        one, two, hit = zero, zero, zero
        for n in range(tiles):
            v = jnp.exp(e_v[r, n * LANES:(n + 1) * LANES] - top)
            e_v[r, n * LANES:(n + 1) * LANES] = v
            one += v
            two += v * v
            hit += jnp.where(lane + n * LANES == lab, v, 0.0)
        one = jnp.sum(one, axis=1, keepdims=True)
        two = jnp.sum(two, axis=1, keepdims=True)
        hit = jnp.sum(hit, axis=1, keepdims=True)
        pick = jnp.where(lane == 4 * h, top, 0.0)
        pick = jnp.where(lane == 4 * h + 1, one, pick)
        pick = jnp.where(lane == 4 * h + 2, two, pick)
        pick = jnp.where(lane == 4 * h + 3, hit, pick)
        xt_v[blk, s * 64:(s + 1) * 64, :] += pick

    def squares_of(blk, i):
        h, s = i // 2, i % 2
        r = slice(blk * WIDE + i * 64, blk * WIDE + (i + 1) * 64)
        sq = jnp.zeros((64, LANES), F32)
        for k in range(depth // LANES):
            v = f_v[r, k * LANES:(k + 1) * LANES].astype(F32)
            sq += v * v
        pick = jnp.where(lane == 8 + h, jnp.sum(sq, axis=1, keepdims=True), 0.0)
        if h == 0:
            xt_v[blk, s * 64:(s + 1) * 64, :] = pick
        else:
            xt_v[blk, s * 64:(s + 1) * 64, :] += pick

    def labels_of(blk):
        if blk == 0:
            lab_load.wait()
        for i in (2 * blk, 2 * blk + 1):
            row = jnp.broadcast_to(labrow_v[i:i + 1, :].astype(F32), (LANES, LANES))
            lab_v[i * LANES:(i + 1) * LANES, :] = row.T.astype(jnp.int32) - z * width

    def turn(i):
        ft_v[:, i * LANES:(i + 1) * LANES] = f_v[i * LANES:(i + 1) * LANES, :].T

    def forward(blk):
        r = slice(blk * WIDE, (blk + 1) * WIDE)
        if blk < blocks:
            with jax.named_scope("load"):
                f_load(blk).wait()
            with jax.named_scope("labels"):
                labels_of(blk)
        if blk == 0:
            for i in range(1, blocks):
                f_load(i).start()
            for i, (k, nk) in enumerate(parts):
                w_load(i).wait()
                for n, w in w_tiles:
                    v = jnp.dot(f_v[r, k:k + nk], w_v[k:k + nk, n:n + w], preferred_element_type=F32)
                    e_v[r, n:n + w] = v if i == 0 else v + e_v[r, n:n + w]
        for i, (n, w) in enumerate(w_tiles):
            if 0 < blk < blocks:
                e_v[r, n:n + w] = jnp.dot(f_v[r, :], w_v[:, n:n + w], preferred_element_type=F32)
            if blk > 0 and i < 4:
                sums(blk - 1, i)
            if blk < blocks and i < 4:
                squares_of(blk, i)
            if 0 < blk < blocks and i >= 4:
                turn((blk - 1) * 2 + i - 4)
        if blk == 0:
            own_load.start()
            nz_load.start()
        if blk == 1:
            pl.semaphore_wait(barrier, 7 + n_cls - 1)
        if blk > 0:
            t = xt_v[blk - 1].T
            st_v[z, blk - 1] = t[0:8]
            fn_v[blk - 1] = t[8:16]
            for k in range(1, n_cls):
                st_copy(blk - 1, k).start()

    for blk in range(blocks + 1):
        with jax.named_scope(f"forward_{blk}"):
            forward(blk)

    with jax.named_scope("turn"):
        nz = send(noise_hbm, nz_v.at[core], nz_s, nz_r, partner)
        nz.start()

        for i in (2 * blocks - 2, 2 * blocks - 1):
            turn(i)

    def weigh(blk, _):
        ref = st_v.at[pl.ds(0, n_cls - 1), blk]
        send(ref, ref, st_s, st_r.at[blk], partner).wait_recv()
        for h in range(2):
            tops = [st_v[p, blk, 4 * h:4 * h + 1, :] for p in range(n_cls)]
            top = functools.reduce(jnp.maximum, tops)
            total = jnp.zeros((1, LANES), F32)
            squares, hit = total, total
            for p in range(n_cls):
                g = jnp.exp(tops[p] - top)
                total += st_v[p, blk, 4 * h + 1:4 * h + 2, :] * g
                squares += st_v[p, blk, 4 * h + 2:4 * h + 3, :] * (g * g)
                hit += st_v[p, blk, 4 * h + 3:4 * h + 4, :] * g
            prob = hit / total
            miss = 1.0 - prob
            resid = jnp.maximum(squares / (total * total) - prob * prob, 0.0) + miss * miss
            norm = jnp.sqrt(fn_v[blk, h:h + 1, :]) * jnp.sqrt(resid)
            factor = CLIP / jnp.maximum(norm, CLIP)
            up = factor * jnp.exp(st_v[z, blk, 4 * h:4 * h + 1, :] - top) / total
            up = jnp.broadcast_to(up, (LANES, LANES)).T
            down = jnp.broadcast_to(factor, (LANES, LANES)).T
            for s in range(2):
                r = pl.ds(pl.multiple_of(blk * WIDE + h * 128 + s * 64, 64), 64)
                lab = lab_v[r, :]
                u, d = up[s * 64:(s + 1) * 64], down[s * 64:(s + 1) * 64]
                for n in range(tiles):
                    v = e_v[r, n * LANES:(n + 1) * LANES] * u
                    v -= jnp.where(lane + n * LANES == lab, d, 0.0)
                    coef_v[n // 2, r, (n % 2) * LANES:(n % 2 + 1) * LANES] = v.astype(BF16)
        return 0

    half = depth // 2

    def p_send(k, i):
        r = pl.ds(pl.multiple_of(i * half, 16), half)
        return send(psend_v.at[k, r, :], precv_v.at[k, r, :], p_s, p_r.at[k, i], partner)

    def strip(i, m):
        return pl.ds(pl.multiple_of(i * half + m * 416, 16), 416)

    early = rows // 2

    def begin():
        def body(i, _):
            for m in range(2):
                acc_v[strip(i, m), :] = jnp.dot(
                    ft_v[strip(i, m), 0:early], coef_v[(1 - c) * 3, 0:early, :], preferred_element_type=F32)
            return 0
        lax.fori_loop(0, 2, body, 0)

    def part(k):
        def body(i, _):
            for m in range(2):
                r0 = early if k == 0 else 0
                v = jnp.dot(ft_v[strip(i, m), r0:rows], coef_v[(1 - c) * 3 + k, r0:rows, :], preferred_element_type=F32)
                psend_v[k, strip(i, m), :] = (v + acc_v[strip(i, m), :] if k == 0 else v).astype(BF16)
            p_send(k, i).start()
            return 0
        lax.fori_loop(0, 2, body, 0)

    def own(k):
        def body(i, _):
            p_send(k, i).wait_recv()
            for m in range(2):
                acc = jnp.dot(ft_v[strip(i, m), :], coef_v[c * 3 + k], preferred_element_type=F32)
                acc += precv_v[k, strip(i, m), :].astype(F32)
                for n in range(4):
                    q = spot(2 * i + m, n)
                    for h in range(2):
                        g_v[2 * k + h, q // 4, q % 4] = acc[
                            n * 104:(n + 1) * 104, h * LANES:(h + 1) * LANES].astype(BF16)
            return 0
        lax.fori_loop(0, 2, body, 0)

    with jax.named_scope("weigh012"):
        lax.fori_loop(0, 2, weigh, 0)
    with jax.named_scope("begin"):
        begin()
    with jax.named_scope("weigh2"):
        weigh(2, 0)
    with jax.named_scope("base"):
        own_load.wait()
        nz_load.wait()
        nz.wait_recv()
        for n in range(tiles):
            cols = slice(n * LANES, (n + 1) * LANES)
            base_v[n] = wown_v[:, cols].astype(F32)
            for i in range(2):
                base_v[n, i * 52:(i + 1) * 52] -= (scale * 0.96 * CLIP) * nz_v[i, :, cols].astype(F32)
    with jax.named_scope("weigh3"):
        weigh(blocks - 1, 0)

    def arrived(ref, j, k):
        send(ref, ref, out_s.at[0], in_r.at[j, k], partner).wait_recv()

    def a_msg(j, k):
        group, hf, t = ((a_op, 0, to_aup), (a_op, 1, to_adn), (a_up, 1, to_aup),
                        (a_dn, 0, to_adn), (a_up, 0, to_aup), (a_dn, 1, to_adn))[k]
        return send(g_v.at[j, group, pl.ds(2 * hf, 2)], ra_v.at[j, pl.ds(2 * k, 2)], out_s.at[0], in_r.at[j, 0 if k < 2 else 1], t)

    def a_far(j, k):
        group, t = ((a_op, to_aop), (a_up, to_aup), (a_dn, to_adn))[k]
        return send(g_v.at[j, group], ra_v.at[j, pl.ds(4 * k, 4)], out_s.at[0], in_r.at[j, min(k, 1)], t)

    def b_far(j, k):
        piece, t = ((b_op, to_bop), (b_up, to_bup), (b_dn, to_bdn))[k]
        return send(hs_v.at[j, piece], rf_v.at[j, k], out_s.at[1], in_r.at[j, 2 + min(k, 1)], t)

    def b_msg(j, k):
        piece, hf, t = ((b_op, 0, to_bup), (b_op, 1, to_bdn), (b_up, 1, to_bup),
                        (b_dn, 0, to_bdn), (b_up, 0, to_bup), (b_dn, 1, to_bdn))[k]
        r0, nr = ROWS[hf]
        return send(hs_v.at[j, piece, pl.ds(r0, nr)], rb_v.at[j, k, pl.ds(0, nr)],
                    out_s.at[1], in_r.at[j, 2 if k < 2 else 3], t)

    def opp(j):
        if j in FAR_RS_A:
            a_far(j, 0).start()
            return
        a_msg(j, 0).start()
        a_msg(j, 1).start()

    def ind(j):
        if j in FAR_RS_A:
            a_far(j, 1).start()
            a_far(j, 2).start()
            return
        a_msg(j, 2).start()
        a_msg(j, 3).start()

    def r1(j):
        if j in FAR_RS_A:
            return
        arrived(ra_v.at[j, pl.ds(0, 4)], j, 0)
        for k, group, hf in ((0, a_up, 0), (1, a_dn, 1)):
            for i in range(2):
                v = g_v[j, group, 2 * hf + i].astype(F32) + ra_v[j, 2 * k + i].astype(F32)
                g_v[j, group, 2 * hf + i] = v.astype(BF16)
            a_msg(j, 4 + k).start()

    def r2(j):
        if j in FAR_RS_A:
            arrived(ra_v.at[j, pl.ds(0, 4)], j, 0)
        arrived(ra_v.at[j, pl.ds(4, 8)], j, 1)
        for i in range(4):
            v = g_v[j, a, i].astype(F32)
            for k in (i, 4 + i, 8 + i) if j in FAR_RS_A else ((8 + i, 6 + i) if i < 2 else (8 + i, 2 + i)):
                v += ra_v[j, k].astype(F32)
            hf_v[j, i] = v
            hs_v[j, i] = v.astype(BF16)
        for k in range(3 if j in FAR_RS_B else 4):
            (b_far if j in FAR_RS_B else b_msg)(j, k).start()

    def r3(j):
        if j in FAR_RS_B:
            return
        arrived(hs_v.at[j, 0], j, 2)
        for k, piece, hf in ((0, b_up, 0), (1, b_dn, 1)):
            r0, nr = ROWS[hf]
            v = hf_v[j, piece, r0:r0 + nr] + rb_v[j, k, 0:nr].astype(F32)
            hs_v[j, piece, r0:r0 + nr] = v.astype(BF16)
            b_msg(j, 4 + k).start()

    def cols(j):
        return pl.ds(pl.multiple_of((c * 6 + j) * LANES, LANES), LANES)

    def place(j, p, hf=None):
        if hf is None:
            return out_ref.at[p, :, cols(j)]
        return out_ref.at[p, pl.ds(*ROWS[hf]), cols(j)]

    def g1(j, k):
        piece, hf, t = ((mine, None, to_bup), (mine, None, to_bdn),
                        (spot(a, b_dn), 0, to_bup), (spot(a, b_up), 1, to_bdn))[k]
        ref = place(j, piece, hf)
        return send(ref, ref, out_s.at[2], in_r.at[j, 4 if k < 2 else 5], t)

    near = (b, b_dn, b_up, b_op)

    def g2(j, r, up):
        ref = place(j, spot(a, near[r]))
        return send(ref, ref, out_s.at[3], in_r.at[j, 6 + r], to_aup if up else to_adn)

    def g3(j, r):
        ref = place(j, spot(a_dn if r < 1 else a_up, near[r]))
        return send(ref, ref, out_s.at[4], in_r.at[j, 10], to_aup if r < 1 else to_adn)

    def d2d(j, i, r):
        ref = place(j, spot((a, a_dn, a_up, a_op)[i], near[r]))
        return send(ref, ref, out_s.at[5], in_r.at[j, 11], partner)

    def have(j, r):
        g2(j, r, 1).start()
        g2(j, r, 0).start()
        if j in FAR_AG_A:
            ref = place(j, spot(a, near[r]))
            send(ref, ref, out_s.at[4], in_r.at[j, 10], to_aop).start()
        d2d(j, 0, r).start()

    def u(j):
        if j in FAR_RS_B:
            arrived(hs_v.at[j, 0], j, 2)
        arrived(hs_v.at[j, pl.ds(0, 2)], j, 3)
        for hf, dep, alone in ((0, 4, 3), (1, 5, 2)):
            r0, nr = ROWS[hf]
            v = hf_v[j, b, r0:r0 + nr]
            if j in FAR_RS_B:
                for k in range(3):
                    v += rf_v[j, k, r0:r0 + nr].astype(F32)
            else:
                v += rb_v[j, dep, 0:nr].astype(F32)
                v += rb_v[j, alone, 0:nr].astype(F32)
            v = base_v[c * 6 + j, r0:r0 + nr] - scale * v
            out_ref[mine, r0:r0 + nr, cols(j)] = v.astype(BF16)
        g1(j, 0).start()
        g1(j, 1).start()
        if j in FAR_AG_B:
            ref = place(j, mine)
            send(ref, ref, out_s.at[2], in_r.at[j, 5], to_bop).start()
        have(j, 0)

    def a1(j):
        arrived(hs_v.at[j, pl.ds(0, 2)], j, 4)
        if j not in FAR_AG_B:
            g1(j, 2).start()
            g1(j, 3).start()
        have(j, 1)
        have(j, 2)

    def a2(j):
        arrived(hs_v.at[j, 0], j, 5)
        have(j, 3)

    def a3(j):
        for r in range(4):
            arrived(hs_v.at[j, pl.ds(0, 2)], j, 6 + r)
            if j not in FAR_AG_A:
                g3(j, r).start()
            d2d(j, 1, r).start()
            d2d(j, 2, r).start()

    def a4(j):
        arrived(hs_v.at[j], j, 10)
        for r in range(4):
            d2d(j, 3, r).start()

    def run(fn, j, role=0):
        with jax.named_scope(f"{fn.__name__}_{j}"):
            if j < 5:
                fn(j)
            else:
                pl.when(c == role)(lambda: fn(j))

    stages = dict(part=part, own=own, opp=opp, ind=ind, r1=r1, r2=r2, r3=r3, u=u, a1=a1, a2=a2, a3=a3, a4=a4)
    for word in ORDER.split():
        name, j = word[:-1], int(word[-1])
        if name in ("part", "own"):
            with jax.named_scope(word):
                stages[name](j)
        else:
            run(stages[name], j)

    def drain(n):
        for k, ref in enumerate((ra_v.at[pl.ds(0, n)], hs_v.at[pl.ds(0, n), pl.ds(0, 3)], hs_v.at[pl.ds(0, n), pl.ds(0, 3)],
                                 g_v.at[pl.ds(0, n), pl.ds(0, 2)], hs_v.at[pl.ds(0, n)], g_v.at[pl.ds(0, n)])):
            send(ref, ref, out_s.at[k], in_r.at[0, 0], partner).wait_send()

    with jax.named_scope("partner"):
        for j in range(6):
            run(lambda k: arrived(g_v.at[k], k, 11), j, 1)
    with jax.named_scope("drain"):
        pl.when(c == 0)(lambda: drain(6))
        pl.when(c == 1)(lambda: drain(5))
    nz.wait_send()
    send(psend_v, precv_v, p_s, p_r.at[0, 0], partner).wait_send()
    ref = st_v.at[pl.ds(0, n_cls - 1)]
    send(ref, ref, st_s, st_r.at[0], partner).wait_send()


def local(features, labels, weight, noise):
    rows, depth = features.shape
    width = weight.shape[1]
    n_cls = lax.axis_size("cls")
    scale = 0.1 * (width * n_cls) / (rows * lax.axis_size("ex"))
    hbm = pl.BlockSpec(memory_space=pltpu.HBM)
    dma = pltpu.SemaphoreType.DMA
    blocks = rows // WIDE
    args = [pltpu.with_memory_space_constraint(v, pltpu.HBM)
            for v in (features, labels.reshape(rows // LANES, LANES), weight, noise)]
    out = pl.pallas_call(
        functools.partial(kernel, scale),
        out_shape=jax.ShapeDtypeStruct((16, 104, width), BF16),
        in_specs=[hbm] * 4,
        out_specs=pl.BlockSpec(memory_space=pltpu.VMEM),
        scratch_shapes=[
            pltpu.VMEM((rows, depth), BF16),
            pltpu.VMEM((depth, width), BF16),
            pltpu.VMEM((depth, rows), BF16),
            pltpu.VMEM((rows, width), F32),
            pltpu.VMEM((6, rows, WIDE), BF16),
            pltpu.VMEM((rows, LANES), jnp.int32),
            pltpu.VMEM((rows // LANES, LANES), jnp.int32),
            pltpu.VMEM((blocks, LANES, LANES), F32),
            pltpu.VMEM((n_cls, blocks, 8, LANES), F32),
            pltpu.VMEM((blocks, 8, LANES), F32),
            pltpu.VMEM((3, depth, WIDE), BF16),
            pltpu.VMEM((3, depth, WIDE), BF16),
            pltpu.VMEM((depth, WIDE), F32),
            pltpu.VMEM((6, 4, 4, 104, LANES), BF16),
            pltpu.VMEM((6, 12, 104, LANES), BF16),
            pltpu.VMEM((6, 4, 104, LANES), F32),
            pltpu.VMEM((6, 4, 104, LANES), BF16),
            pltpu.VMEM((6, 6, 56, LANES), BF16),
            pltpu.VMEM((6, 3, 104, LANES), BF16),
            pltpu.VMEM((width // LANES, 104, LANES), F32),
            pltpu.VMEM((104, width), BF16),
            pltpu.VMEM((2, 52, width), BF16),
            dma((3,)), dma((2,)), dma((blocks,)), dma, dma((blocks,)), dma, dma,
            dma, dma((3, 2)), dma((6,)), dma((6, 12)),
        ],
        compiler_params=pltpu.CompilerParams(
            collective_id=0, has_side_effects=True, vmem_limit_bytes=48_000_000),
        cost_estimate=pl.CostEstimate(flops=4 * rows * depth * width, bytes_accessed=16_000_000,
                                      transcendentals=rows * width),
    )(*args)
    return out.reshape(depth, width)


def solution(mesh):
    in_specs = (P("ex", None), P("ex"), P(None, "cls"), P("ex", "cls"))
    out_specs = P(None, "cls")
    return jax.shard_map(local, mesh=mesh, in_specs=in_specs, out_specs=out_specs, check_vma=False)
```

```python
import functools

import jax
import jax.numpy as jnp
from jax import lax
from jax.experimental import pallas as pl
from jax.experimental.pallas import tpu as pltpu
from jax.sharding import PartitionSpec as P

MESH = pl.DeviceIdType.MESH
F32, BF16 = jnp.float32, jnp.bfloat16
CLIP = 48.0
WIDE = 256
LANES = 128
ROWS = ((0, 48), (48, 56))

ORDER = " ".join((
    "part0 part1 own0 opp1", "opp0 ind0 own1 ind1", "opp3 opp2 part2 ind2",
    "ind3 r11 r10 own2", "opp5 opp4 r13 r12", "r21 r31 ind4 r15",
    "r14 r23 ind5 r20", "r22 r33 r30 u1", "r24 r25 u3 r35",
    "u0 a11 r32 u5", "u2 a13 r34 a21", "u4 a15 a12 a22",
    "a10 a20 a23 a31", "a25 a14 a24 a32", "a30 a35 a33 a42",
    "a34 a41 a40 a44", "a45 a43",
))
FAR_RS_A = ()
FAR_RS_B = (0, 1, 2, 3, 4, 5)
FAR_AG_B = (0, 2, 4)
FAR_AG_A = (4,)


def kernel(scale, f_hbm, lab_hbm, w_hbm, noise_hbm, out_ref,
           f_v, w_v, ft_v, e_v, coef_v, lab_v, labrow_v, xt_v, st_v, fn_v, psend_v, precv_v, acc_v,
           g_v, ra_v, hf_v, hs_v, rb_v, rf_v, base_v, wown_v, nz_v,
           ld_sem, w_sem, f_sem, st_s, st_r, nz_s, nz_r, p_s, p_r, out_s, in_r):
    rows, depth = f_hbm.shape
    width = w_hbm.shape[1]
    tiles = width // LANES
    blocks = rows // WIDE
    n_cls = lax.axis_size("cls")
    ex = lax.axis_index("ex")
    z = lax.axis_index("cls")
    core = ex % 2
    c = 1 - core
    x = ex // 8
    y = (ex // 2) % 4
    a = x * (1 - c) + y * c
    b = y * (1 - c) + x * c

    def spot(i, j):
        return i * (4 - 3 * c) + j * (1 + 3 * c)

    def dev(i, j):
        return spot(i, j) * 2 + core

    mine = spot(a, b)
    a_up, a_dn, a_op = (a + 1) % 4, (a + 3) % 4, (a + 2) % 4
    b_up, b_dn, b_op = (b + 1) % 4, (b + 3) % 4, (b + 2) % 4
    to_aup, to_adn = dev(a_up, b), dev(a_dn, b)
    to_bup, to_bdn = dev(a, b_up), dev(a, b_dn)
    to_aop, to_bop = dev(a_op, b), dev(a, b_op)
    partner = ex + 1 - 2 * core

    w_tiles = [(n, min(WIDE, width - n)) for n in range(0, width, WIDE)]

    def f_load(i):
        r = pl.ds(i * WIDE, WIDE)
        return pltpu.make_async_copy(f_hbm.at[r, :], f_v.at[r, :], f_sem.at[i])

    parts = ((0, 768), (768, depth - 768))

    def w_load(i):
        r = pl.ds(*parts[i])
        return pltpu.make_async_copy(w_hbm.at[r, :], w_v.at[r, :], w_sem.at[i])

    lab_load = pltpu.make_async_copy(lab_hbm, labrow_v, ld_sem.at[0])
    own_load = pltpu.make_async_copy(
        w_hbm.at[pl.ds(pl.multiple_of(mine * 104, 8), 104), :], wown_v, ld_sem.at[1])
    nz_load = pltpu.make_async_copy(noise_hbm, nz_v.at[core], ld_sem.at[2])
    lab_load.start()
    f_load(0).start()
    w_load(0).start()
    w_load(1).start()

    barrier = pltpu.get_barrier_semaphore()
    for t in (to_aup, to_adn, to_aop, to_bup, to_bdn, to_bop, partner):
        pl.semaphore_signal(barrier, inc=1, device_id={"ex": t}, device_id_type=MESH)
    for k in range(1, n_cls):
        pl.semaphore_signal(barrier, inc=1, device_id={"cls": (z + k) % n_cls}, device_id_type=MESH)

    def send(src, dst, s, r, t):
        return pltpu.make_async_remote_copy(
            src_ref=src, dst_ref=dst, send_sem=s, recv_sem=r, device_id={"ex": t}, device_id_type=MESH)

    coef_v[5, :, LANES:] = jnp.zeros((rows, LANES), BF16)
    lane = lax.broadcasted_iota(jnp.int32, (64, LANES), 1)

    def st_copy(blk, k):
        return pltpu.make_async_remote_copy(
            src_ref=st_v.at[z, blk], dst_ref=st_v.at[z, blk], send_sem=st_s, recv_sem=st_r.at[blk], device_id={"cls": (z + k) % n_cls}, device_id_type=MESH)

    def sums(blk, i):
        h, s = i // 2, i % 2
        r = slice(blk * WIDE + i * 64, blk * WIDE + (i + 1) * 64)
        top = e_v[r, 0:LANES]
        for n in range(1, tiles):
            top = jnp.maximum(top, e_v[r, n * LANES:(n + 1) * LANES])
        top = jnp.max(top, axis=1, keepdims=True)
        lab = lab_v[r, :]
        zero = jnp.zeros((64, LANES), F32)
        one, two, hit = zero, zero, zero
        for n in range(tiles):
            v = jnp.exp(e_v[r, n * LANES:(n + 1) * LANES] - top)
            e_v[r, n * LANES:(n + 1) * LANES] = v
            one += v
            two += v * v
            hit += jnp.where(lane + n * LANES == lab, v, 0.0)
        one = jnp.sum(one, axis=1, keepdims=True)
        two = jnp.sum(two, axis=1, keepdims=True)
        hit = jnp.sum(hit, axis=1, keepdims=True)
        pick = jnp.where(lane == 4 * h, top, 0.0)
        pick = jnp.where(lane == 4 * h + 1, one, pick)
        pick = jnp.where(lane == 4 * h + 2, two, pick)
        pick = jnp.where(lane == 4 * h + 3, hit, pick)
        xt_v[blk, s * 64:(s + 1) * 64, :] += pick

    def squares_of(blk, i):
        h, s = i // 2, i % 2
        r = slice(blk * WIDE + i * 64, blk * WIDE + (i + 1) * 64)
        sq = jnp.zeros((64, LANES), F32)
        for k in range(depth // LANES):
            v = f_v[r, k * LANES:(k + 1) * LANES].astype(F32)
            sq += v * v
        pick = jnp.where(lane == 8 + h, jnp.sum(sq, axis=1, keepdims=True), 0.0)
        if h == 0:
            xt_v[blk, s * 64:(s + 1) * 64, :] = pick
        else:
            xt_v[blk, s * 64:(s + 1) * 64, :] += pick

    def labels_of(blk):
        if blk == 0:
            lab_load.wait()
        for i in (2 * blk, 2 * blk + 1):
            row = jnp.broadcast_to(labrow_v[i:i + 1, :].astype(F32), (LANES, LANES))
            lab_v[i * LANES:(i + 1) * LANES, :] = row.T.astype(jnp.int32) - z * width

    def turn(i):
        ft_v[:, i * LANES:(i + 1) * LANES] = f_v[i * LANES:(i + 1) * LANES, :].T

    def forward(blk):
        r = slice(blk * WIDE, (blk + 1) * WIDE)
        if blk < blocks:
            with jax.named_scope("load"):
                f_load(blk).wait()
            with jax.named_scope("labels"):
                labels_of(blk)
        if blk == 0:
            for i in range(1, blocks):
                f_load(i).start()
            for i, (k, nk) in enumerate(parts):
                w_load(i).wait()
                for n, w in w_tiles:
                    v = jnp.dot(f_v[r, k:k + nk], w_v[k:k + nk, n:n + w], preferred_element_type=F32)
                    e_v[r, n:n + w] = v if i == 0 else v + e_v[r, n:n + w]
        for i, (n, w) in enumerate(w_tiles):
            if 0 < blk < blocks:
                e_v[r, n:n + w] = jnp.dot(f_v[r, :], w_v[:, n:n + w], preferred_element_type=F32)
            if blk > 0 and i < 4:
                sums(blk - 1, i)
            if blk < blocks and i < 4:
                squares_of(blk, i)
            if 0 < blk < blocks and i >= 4:
                turn((blk - 1) * 2 + i - 4)
        if blk == 0:
            own_load.start()
            nz_load.start()
        if blk == 1:
            pl.semaphore_wait(barrier, 7 + n_cls - 1)
        if blk > 0:
            t = xt_v[blk - 1].T
            st_v[z, blk - 1] = t[0:8]
            fn_v[blk - 1] = t[8:16]
            for k in range(1, n_cls):
                st_copy(blk - 1, k).start()

    for blk in range(blocks + 1):
        with jax.named_scope(f"forward_{blk}"):
            forward(blk)

    with jax.named_scope("turn"):
        nz = send(noise_hbm, nz_v.at[core], nz_s, nz_r, partner)
        nz.start()

        for i in (2 * blocks - 2, 2 * blocks - 1):
            turn(i)

    def weigh(blk, _):
        ref = st_v.at[pl.ds(0, n_cls - 1), blk]
        send(ref, ref, st_s, st_r.at[blk], partner).wait_recv()
        for h in range(2):
            tops = [st_v[p, blk, 4 * h:4 * h + 1, :] for p in range(n_cls)]
            top = functools.reduce(jnp.maximum, tops)
            total = jnp.zeros((1, LANES), F32)
            squares, hit = total, total
            for p in range(n_cls):
                g = jnp.exp(tops[p] - top)
                total += st_v[p, blk, 4 * h + 1:4 * h + 2, :] * g
                squares += st_v[p, blk, 4 * h + 2:4 * h + 3, :] * (g * g)
                hit += st_v[p, blk, 4 * h + 3:4 * h + 4, :] * g
            prob = hit / total
            miss = 1.0 - prob
            resid = jnp.maximum(squares / (total * total) - prob * prob, 0.0) + miss * miss
            norm = jnp.sqrt(fn_v[blk, h:h + 1, :]) * jnp.sqrt(resid)
            factor = CLIP / jnp.maximum(norm, CLIP)
            up = factor * jnp.exp(st_v[z, blk, 4 * h:4 * h + 1, :] - top) / total
            up = jnp.broadcast_to(up, (LANES, LANES)).T
            down = jnp.broadcast_to(factor, (LANES, LANES)).T
            for s in range(2):
                r = pl.ds(pl.multiple_of(blk * WIDE + h * 128 + s * 64, 64), 64)
                lab = lab_v[r, :]
                u, d = up[s * 64:(s + 1) * 64], down[s * 64:(s + 1) * 64]
                for n in range(tiles):
                    v = e_v[r, n * LANES:(n + 1) * LANES] * u
                    v -= jnp.where(lane + n * LANES == lab, d, 0.0)
                    coef_v[n // 2, r, (n % 2) * LANES:(n % 2 + 1) * LANES] = v.astype(BF16)
        return 0

    half = depth // 2

    def p_send(k, i):
        r = pl.ds(pl.multiple_of(i * half, 16), half)
        return send(psend_v.at[k, r, :], precv_v.at[k, r, :], p_s, p_r.at[k, i], partner)

    def strip(i, m):
        return pl.ds(pl.multiple_of(i * half + m * 416, 16), 416)

    early = rows // 2

    def begin():
        def body(i, _):
            for m in range(2):
                acc_v[strip(i, m), :] = jnp.dot(
                    ft_v[strip(i, m), 0:early], coef_v[(1 - c) * 3, 0:early, :], preferred_element_type=F32)
            return 0
        lax.fori_loop(0, 2, body, 0)

    def part(k):
        def body(i, _):
            for m in range(2):
                r0 = early if k == 0 else 0
                v = jnp.dot(ft_v[strip(i, m), r0:rows], coef_v[(1 - c) * 3 + k, r0:rows, :], preferred_element_type=F32)
                psend_v[k, strip(i, m), :] = (v + acc_v[strip(i, m), :] if k == 0 else v).astype(BF16)
            p_send(k, i).start()
            return 0
        lax.fori_loop(0, 2, body, 0)

    def own(k):
        def body(i, _):
            p_send(k, i).wait_recv()
            for m in range(2):
                acc = jnp.dot(ft_v[strip(i, m), :], coef_v[c * 3 + k], preferred_element_type=F32)
                acc += precv_v[k, strip(i, m), :].astype(F32)
                for n in range(4):
                    q = spot(2 * i + m, n)
                    for h in range(2):
                        g_v[2 * k + h, q // 4, q % 4] = acc[
                            n * 104:(n + 1) * 104, h * LANES:(h + 1) * LANES].astype(BF16)
            return 0
        lax.fori_loop(0, 2, body, 0)

    with jax.named_scope("weigh012"):
        lax.fori_loop(0, 2, weigh, 0)
    with jax.named_scope("begin"):
        begin()
    with jax.named_scope("weigh2"):
        weigh(2, 0)
    with jax.named_scope("base"):
        own_load.wait()
        nz_load.wait()
        nz.wait_recv()
        for n in range(tiles):
            cols = slice(n * LANES, (n + 1) * LANES)
            base_v[n] = wown_v[:, cols].astype(F32)
            for i in range(2):
                base_v[n, i * 52:(i + 1) * 52] -= (scale * 0.96 * CLIP) * nz_v[i, :, cols].astype(F32)
    with jax.named_scope("weigh3"):
        weigh(blocks - 1, 0)

    def arrived(ref, j, k):
        send(ref, ref, out_s.at[0], in_r.at[j, k], partner).wait_recv()

    def a_msg(j, k):
        group, hf, t = ((a_op, 0, to_aup), (a_op, 1, to_adn), (a_up, 1, to_aup),
                        (a_dn, 0, to_adn), (a_up, 0, to_aup), (a_dn, 1, to_adn))[k]
        return send(g_v.at[j, group, pl.ds(2 * hf, 2)], ra_v.at[j, pl.ds(2 * k, 2)], out_s.at[0], in_r.at[j, 0 if k < 2 else 1], t)

    def a_far(j, k):
        group, t = ((a_op, to_aop), (a_up, to_aup), (a_dn, to_adn))[k]
        return send(g_v.at[j, group], ra_v.at[j, pl.ds(4 * k, 4)], out_s.at[0], in_r.at[j, min(k, 1)], t)

    def b_far(j, k):
        piece, t = ((b_op, to_bop), (b_up, to_bup), (b_dn, to_bdn))[k]
        return send(hs_v.at[j, piece], rf_v.at[j, k], out_s.at[1], in_r.at[j, 2 + min(k, 1)], t)

    def b_msg(j, k):
        piece, hf, t = ((b_op, 0, to_bup), (b_op, 1, to_bdn), (b_up, 1, to_bup),
                        (b_dn, 0, to_bdn), (b_up, 0, to_bup), (b_dn, 1, to_bdn))[k]
        r0, nr = ROWS[hf]
        return send(hs_v.at[j, piece, pl.ds(r0, nr)], rb_v.at[j, k, pl.ds(0, nr)],
                    out_s.at[1], in_r.at[j, 2 if k < 2 else 3], t)

    def opp(j):
        if j in FAR_RS_A:
            a_far(j, 0).start()
            return
        a_msg(j, 0).start()
        a_msg(j, 1).start()

    def ind(j):
        if j in FAR_RS_A:
            a_far(j, 1).start()
            a_far(j, 2).start()
            return
        a_msg(j, 2).start()
        a_msg(j, 3).start()

    def r1(j):
        if j in FAR_RS_A:
            return
        arrived(ra_v.at[j, pl.ds(0, 4)], j, 0)
        for k, group, hf in ((0, a_up, 0), (1, a_dn, 1)):
            for i in range(2):
                v = g_v[j, group, 2 * hf + i].astype(F32) + ra_v[j, 2 * k + i].astype(F32)
                g_v[j, group, 2 * hf + i] = v.astype(BF16)
            a_msg(j, 4 + k).start()

    def r2(j):
        if j in FAR_RS_A:
            arrived(ra_v.at[j, pl.ds(0, 4)], j, 0)
        arrived(ra_v.at[j, pl.ds(4, 8)], j, 1)
        for i in range(4):
            v = g_v[j, a, i].astype(F32)
            for k in (i, 4 + i, 8 + i) if j in FAR_RS_A else ((8 + i, 6 + i) if i < 2 else (8 + i, 2 + i)):
                v += ra_v[j, k].astype(F32)
            hf_v[j, i] = v
            hs_v[j, i] = v.astype(BF16)
        for k in range(3 if j in FAR_RS_B else 4):
            (b_far if j in FAR_RS_B else b_msg)(j, k).start()

    def r3(j):
        if j in FAR_RS_B:
            return
        arrived(hs_v.at[j, 0], j, 2)
        for k, piece, hf in ((0, b_up, 0), (1, b_dn, 1)):
            r0, nr = ROWS[hf]
            v = hf_v[j, piece, r0:r0 + nr] + rb_v[j, k, 0:nr].astype(F32)
            hs_v[j, piece, r0:r0 + nr] = v.astype(BF16)
            b_msg(j, 4 + k).start()

    def cols(j):
        return pl.ds(pl.multiple_of((c * 6 + j) * LANES, LANES), LANES)

    def place(j, p, hf=None):
        if hf is None:
            return out_ref.at[p, :, cols(j)]
        return out_ref.at[p, pl.ds(*ROWS[hf]), cols(j)]

    def g1(j, k):
        piece, hf, t = ((mine, None, to_bup), (mine, None, to_bdn),
                        (spot(a, b_dn), 0, to_bup), (spot(a, b_up), 1, to_bdn))[k]
        ref = place(j, piece, hf)
        return send(ref, ref, out_s.at[2], in_r.at[j, 4 if k < 2 else 5], t)

    near = (b, b_dn, b_up, b_op)

    def g2(j, r, up):
        ref = place(j, spot(a, near[r]))
        return send(ref, ref, out_s.at[3], in_r.at[j, 6 + r], to_aup if up else to_adn)

    def g3(j, r):
        ref = place(j, spot(a_dn if r < 1 else a_up, near[r]))
        return send(ref, ref, out_s.at[4], in_r.at[j, 10], to_aup if r < 1 else to_adn)

    def d2d(j, i, r):
        ref = place(j, spot((a, a_dn, a_up, a_op)[i], near[r]))
        return send(ref, ref, out_s.at[5], in_r.at[j, 11], partner)

    def have(j, r):
        g2(j, r, 1).start()
        g2(j, r, 0).start()
        if j in FAR_AG_A:
            ref = place(j, spot(a, near[r]))
            send(ref, ref, out_s.at[4], in_r.at[j, 10], to_aop).start()
        d2d(j, 0, r).start()

    def u(j):
        if j in FAR_RS_B:
            arrived(hs_v.at[j, 0], j, 2)
        arrived(hs_v.at[j, pl.ds(0, 2)], j, 3)
        for hf, dep, alone in ((0, 4, 3), (1, 5, 2)):
            r0, nr = ROWS[hf]
            v = hf_v[j, b, r0:r0 + nr]
            if j in FAR_RS_B:
                for k in range(3):
                    v += rf_v[j, k, r0:r0 + nr].astype(F32)
            else:
                v += rb_v[j, dep, 0:nr].astype(F32)
                v += rb_v[j, alone, 0:nr].astype(F32)
            v = base_v[c * 6 + j, r0:r0 + nr] - scale * v
            out_ref[mine, r0:r0 + nr, cols(j)] = v.astype(BF16)
        g1(j, 0).start()
        g1(j, 1).start()
        if j in FAR_AG_B:
            ref = place(j, mine)
            send(ref, ref, out_s.at[2], in_r.at[j, 5], to_bop).start()
        have(j, 0)

    def a1(j):
        arrived(hs_v.at[j, pl.ds(0, 2)], j, 4)
        if j not in FAR_AG_B:
            g1(j, 2).start()
            g1(j, 3).start()
        have(j, 1)
        have(j, 2)

    def a2(j):
        arrived(hs_v.at[j, 0], j, 5)
        have(j, 3)

    def a3(j):
        for r in range(4):
            arrived(hs_v.at[j, pl.ds(0, 2)], j, 6 + r)
            if j not in FAR_AG_A:
                g3(j, r).start()
            d2d(j, 1, r).start()
            d2d(j, 2, r).start()

    def a4(j):
        arrived(hs_v.at[j], j, 10)
        for r in range(4):
            d2d(j, 3, r).start()

    def run(fn, j, role=0):
        with jax.named_scope(f"{fn.__name__}_{j}"):
            if j < 5:
                fn(j)
            else:
                pl.when(c == role)(lambda: fn(j))

    stages = dict(part=part, own=own, opp=opp, ind=ind, r1=r1, r2=r2, r3=r3, u=u, a1=a1, a2=a2, a3=a3, a4=a4)
    for word in ORDER.split():
        name, j = word[:-1], int(word[-1])
        if name in ("part", "own"):
            with jax.named_scope(word):
                stages[name](j)
        else:
            run(stages[name], j)

    def drain(n):
        for k, ref in enumerate((ra_v.at[pl.ds(0, n)], hs_v.at[pl.ds(0, n), pl.ds(0, 3)], hs_v.at[pl.ds(0, n), pl.ds(0, 3)],
                                 g_v.at[pl.ds(0, n), pl.ds(0, 2)], hs_v.at[pl.ds(0, n)], g_v.at[pl.ds(0, n)])):
            send(ref, ref, out_s.at[k], in_r.at[0, 0], partner).wait_send()

    with jax.named_scope("partner"):
        for j in range(6):
            run(lambda k: arrived(g_v.at[k], k, 11), j, 1)
    with jax.named_scope("drain"):
        pl.when(c == 0)(lambda: drain(6))
        pl.when(c == 1)(lambda: drain(5))
    nz.wait_send()
    send(psend_v, precv_v, p_s, p_r.at[0, 0], partner).wait_send()
    ref = st_v.at[pl.ds(0, n_cls - 1)]
    send(ref, ref, st_s, st_r.at[0], partner).wait_send()


def local(features, labels, weight, noise):
    rows, depth = features.shape
    width = weight.shape[1]
    n_cls = lax.axis_size("cls")
    scale = 0.1 * (width * n_cls) / (rows * lax.axis_size("ex"))
    hbm = pl.BlockSpec(memory_space=pltpu.HBM)
    dma = pltpu.SemaphoreType.DMA
    blocks = rows // WIDE
    args = [pltpu.with_memory_space_constraint(v, pltpu.HBM)
            for v in (features, labels.reshape(rows // LANES, LANES), weight, noise)]
    out = pl.pallas_call(
        functools.partial(kernel, scale),
        out_shape=jax.ShapeDtypeStruct((16, 104, width), BF16),
        in_specs=[hbm] * 4,
        out_specs=pl.BlockSpec(memory_space=pltpu.VMEM),
        scratch_shapes=[
            pltpu.VMEM((rows, depth), BF16),
            pltpu.VMEM((depth, width), BF16),
            pltpu.VMEM((depth, rows), BF16),
            pltpu.VMEM((rows, width), F32),
            pltpu.VMEM((6, rows, WIDE), BF16),
            pltpu.VMEM((rows, LANES), jnp.int32),
            pltpu.VMEM((rows // LANES, LANES), jnp.int32),
            pltpu.VMEM((blocks, LANES, LANES), F32),
            pltpu.VMEM((n_cls, blocks, 8, LANES), F32),
            pltpu.VMEM((blocks, 8, LANES), F32),
            pltpu.VMEM((3, depth, WIDE), BF16),
            pltpu.VMEM((3, depth, WIDE), BF16),
            pltpu.VMEM((depth, WIDE), F32),
            pltpu.VMEM((6, 4, 4, 104, LANES), BF16),
            pltpu.VMEM((6, 12, 104, LANES), BF16),
            pltpu.VMEM((6, 4, 104, LANES), F32),
            pltpu.VMEM((6, 4, 104, LANES), BF16),
            pltpu.VMEM((6, 6, 56, LANES), BF16),
            pltpu.VMEM((6, 3, 104, LANES), BF16),
            pltpu.VMEM((width // LANES, 104, LANES), F32),
            pltpu.VMEM((104, width), BF16),
            pltpu.VMEM((2, 52, width), BF16),
            dma((3,)), dma((2,)), dma((blocks,)), dma, dma((blocks,)), dma, dma,
            dma, dma((3, 2)), dma((6,)), dma((6, 12)),
        ],
        compiler_params=pltpu.CompilerParams(
            collective_id=0, has_side_effects=True, vmem_limit_bytes=48_000_000),
        cost_estimate=pl.CostEstimate(flops=4 * rows * depth * width, bytes_accessed=16_000_000,
                                      transcendentals=rows * width),
    )(*args)
    return out.reshape(depth, width)


def solution(mesh):
    in_specs = (P("ex", None), P("ex"), P(None, "cls"), P("ex", "cls"))
    out_specs = P(None, "cls")
    return jax.shard_map(local, mesh=mesh, in_specs=in_specs, out_specs=out_specs, check_vma=False)
```
